32 devices in a mesh: groups: 2 (over y), seq: 4 (over z), tp: 2 (over x), ref: 2 (over core).
Axes of the slice: x: 2, y: 2, z: 4, core: 2. Of those that a mesh axis runs over, the one named last changes fastest.
Arguments:
- hidden: bfloat16 [2, 2048, 4096], P('ref', ('groups', 'seq'), 'tp'), parts along dimension 1, may hold values from -6 to 6
- segment_ids: int32 [2048], P(('groups', 'seq')), parts along dimension 0, may hold values from 0 to 3, never falling along the last dimension, each value on 1 to 768 neighbouring positions
- targets: int32 [2048], P(('groups', 'seq')), parts along dimension 0, may hold values from 0 to 4095
- loss_mask: int32 [2048], P(('groups', 'seq')), parts along dimension 0, may hold values from 0 to 1, as said below
- attn_gain: float32 [2, 4096], P('ref'), may hold values from 0.5 to 2
- final_gain: float32 [2, 4096], P('ref'), may hold values from 1 to 4
- w_query: bfloat16 [2, 4096, 2048], P('ref', 'seq', 'tp'), may hold values from -0.125 to 0.125
- w_key: bfloat16 [2, 4096, 1024], P('ref', 'seq', 'tp'), may hold values from -0.125 to 0.125
- w_value: bfloat16 [2, 4096, 1024], P('ref', 'seq', 'tp'), may hold values from -0.09375 to 0.09375
- w_out: bfloat16 [2, 2048, 4096], P('ref', 'tp', 'seq'), may hold values from -0.125 to 0.125
- head: bfloat16 [2, 4096, 4096], P('ref', None, ('seq', 'tp')), may hold values from -0.25784398 to 0.25784398
Outputs:
- logprobs: float32 [2, 2048], P('ref', ('groups', 'seq')), parts along dimension 1
The draws below stay inside these ranges and needn't reach their ends.
There are 2 independent parts, one for each index of `groups`. The reference program is written for one: setup_inputs(seed, part) draws one part's arguments, and reference() takes and returns one part's arrays. A program takes and returns all parts, laid end to end along the dimension named above; an argument that names none is the same for every part. Nothing has to cross between parts.
Inputs may be any that keep to these rules, and one draw needn't show every extreme that they name: `loss_mask`: each aligned block of 256 positions holds 1 to 32 positions with mask 1, and some block holds exactly 32. `segment_ids`: never falling; every rollout number appears; the longest rollout holds exactly 768 positions.
All inputs are finite; a program needn't handle non-finite values.
Results may differ from the reference program's by a relative error of at most 0.0003.
Values may be sent and summed in bfloat16 or wider, within the bound.
A program may use at most 128 MiB of HBM per device.

```python
import math
import jax
import jax.numpy as jnp
import numpy as np
from jax import lax

D = 4096
KV_HEADS = 8
HEAD_DIM = 128
HEADS = 16
TOK_DEV = 256
WINDOW = 2048
CAP = 32
SEGMENTS = 4
LENGTH = 1024
VOCAB = 4096


def bounded_normal(key, shape, spread, limit):
    return jnp.clip(jax.random.normal(key, shape, jnp.float32), -limit, limit) * spread


def base_noise(key, shape, spread):
    return bounded_normal(key, shape, spread, 4.0)


def draw_loss_mask(key, part):
    blocks = LENGTH // TOK_DEV
    base = jax.random.fold_in(key, 17)
    first, second, third = jax.random.split(base, 3)
    lowest = max(1, CAP // 4)
    counts = jax.random.randint(first, (blocks,), lowest, CAP + 1)
    fullest = jax.random.randint(second, (), 0, blocks)
    counts = jnp.where(jnp.arange(blocks) == fullest, CAP, counts)
    block_keys = jax.random.split(third, blocks)
    orders = jax.vmap(lambda k: jax.random.permutation(k, TOK_DEV))(block_keys)
    chosen = orders < counts[:, None]
    return chosen.astype(jnp.int32).reshape(LENGTH)


def draw_hidden(key, part):
    noise_key, row_key, height_key = jax.random.split(jax.random.fold_in(key, 31), 3)
    shape = (2, LENGTH, D)
    marked = jax.random.randint(row_key, (LENGTH,), 0, 8) == 0
    height = jax.random.uniform(height_key, (LENGTH,), jnp.float32, 2.0, 4.0)
    noise = bounded_normal(noise_key, shape, 1.0, 6.0)
    drawn = jnp.clip(noise, -4.0, 4.0)
    lifted = jnp.where(marked[None, :, None], 0.5 * drawn + height[None, :, None], noise)
    return lifted.astype(jnp.bfloat16)


def drawn_projection(key, heads):
    noise_key, gain_key = jax.random.split(key)
    columns = heads * HEAD_DIM
    spread = D ** (-0.5)
    noise = base_noise(noise_key, (2, D, columns), spread)
    target = jnp.exp(jax.random.uniform(gain_key, (2, heads, 1), jnp.float32, math.log(150.0), math.log(500.0)))
    strength = jnp.sqrt(target / (0.29 * math.sqrt(HEAD_DIM) * D))
    lanes = jnp.arange(HEAD_DIM) % (HEAD_DIM // 2) >= 3 * HEAD_DIM // 8
    column_lift = (strength * lanes.astype(jnp.float32)[None, None, :]).reshape(2, columns) * spread
    return (noise + column_lift[:, None, :]).astype(jnp.bfloat16)


def draw_w_query(key, part):
    return drawn_projection(jax.random.fold_in(key, 53), HEADS)


def draw_w_key(key, part):
    return drawn_projection(jax.random.fold_in(key, 59), KV_HEADS)


def draw_head(key, part):
    noise_key, pick_key, height_key = jax.random.split(jax.random.fold_in(key, 71), 3)
    spread = (D // 9) ** (-0.5)
    shape = (2, D, VOCAB)
    noise = base_noise(noise_key, shape, spread)
    period = min(256, VOCAB // 8)
    offset = jax.random.randint(pick_key, (2, 1), 0, period)
    place = (jnp.arange(VOCAB)[None, :] + offset) % period
    first = place == 0
    second = place == 1
    height = jax.random.uniform(height_key, (2, VOCAB), jnp.float32, 2.0, 4.0)
    partner = jnp.roll(height, 1, axis=1)
    cut = max(1, math.isqrt(D) // 8)
    kept = (jnp.arange(D) >= cut).astype(jnp.float32)[None, :, None]
    lift_first = (height * spread)[:, None, :]
    lift_second = (partner * spread)[:, None, :] * kept
    planted = jnp.where(first[:, None, :], lift_first + 0.25 * noise, jnp.where(second[:, None, :], lift_second + 0.25 * noise, noise))
    return planted.astype(jnp.bfloat16)


def touch_ends(array, own_key, least, top_value):
    index_at = [jax.random.randint(jax.random.fold_in(own_key, axis), (), 0, length) for axis, length in enumerate(array.shape)]
    longest = array.shape.index(max(array.shape))
    next_to = index_at[:longest] + [(index_at[longest] + 1) % array.shape[longest]] + index_at[longest + 1:]
    return array.at[tuple(index_at)].set(least).at[tuple(next_to)].set(top_value)


def shard_levels(rng, extent, cuts, smallest, top_value):
    level, own = 1.0, jax.random.fold_in(rng, 6)
    for axis_at, parts in cuts:
        heights = jnp.exp(jax.random.uniform(jax.random.fold_in(own, axis_at), (parts,), jnp.float32, smallest / len(cuts), top_value / len(cuts)))
        level = level * jnp.repeat(heights, extent[axis_at] // parts).reshape([-1 if axis == axis_at else 1 for axis in range(len(extent))])
    return level


def rank_bounds(amount, lean):
    portions = [(1 << 20) // math.isqrt(grade ** lean) + 1 for grade in range(1, amount + 1)]
    width = 1 + sum(portions) // (1 << 30)
    return np.cumsum(np.array([max(1, weight // width) for weight in portions]))


def skewed_ids(own_key, extent, count, skew):
    grid = rank_bounds(count, skew)
    pick = jax.random.randint(jax.random.fold_in(own_key, 1), extent, 0, int(grid[count - 1]))
    standing = jnp.searchsorted(jnp.asarray(grid, jnp.int32), pick, side="right")
    return jax.random.permutation(jax.random.fold_in(own_key, 2), count)[standing].astype(jnp.int32)


def length_profile(number_of, total, bound, skew):
    portions = [(1 << 20) // math.isqrt(grade ** skew) + 1 for grade in range(2, number_of + 1)]
    spare, given = total - bound - (number_of - 1), [1] * (number_of - 1)
    while spare > 0:
        free = [i for i in range(number_of - 1) if given[i] < bound]
        whole, left = sum([portions[i] for i in free]), spare
        for i in free:
            extra = min(bound - given[i], max(1, left * portions[i] // whole), spare)
            given[i] = given[i] + extra
            spare = spare - extra
    return np.array([bound] + given)


def uneven_parts(rng, amount, total, reach, lean):
    if amount == 2:
        one = jax.random.randint(rng, (), max(1, total - reach), min(reach, total - 1) + 1)
        return jnp.stack([one, total - one])
    tallies = jnp.asarray(length_profile(amount, total, reach, lean), jnp.int32)
    twos = (amount - 1) // 2
    giver, taker = tallies[1:1 + 2 * twos:2], tallies[2:2 + 2 * twos:2]
    margin = jnp.minimum(giver - 1, reach - taker)
    moved = jax.random.randint(jax.random.fold_in(rng, 1), (twos,), 0, 1 << 20) % (margin + 1)
    tallies = tallies.at[1:1 + 2 * twos:2].set(giver - moved).at[2:2 + 2 * twos:2].set(taker + moved)
    return tallies[jax.random.permutation(jax.random.fold_in(rng, 2), amount)]


def normal_values(own_key, extent, scale, most, shards=(), held_as=jnp.bfloat16):
    loudness = shard_levels(own_key, extent, shards, -0.22, 0.18) if shards else 1.0
    array = jax.random.normal(own_key, extent, jnp.float32) * scale * loudness
    return jnp.minimum(jnp.maximum(array, -most), most).astype(held_as)


def setup_inputs(seed: int = 0, part: int = 0) -> dict:
    key_list = jax.random.split(jax.random.key(seed), 12)
    own_keys = jax.random.split(jax.random.fold_in(key_list[11], part), 12)
    hidden = draw_hidden(jax.random.fold_in(jax.random.fold_in(key_list[11], part), 71), part)
    segment_ids = jnp.searchsorted(jnp.cumsum(uneven_parts(own_keys[1], SEGMENTS, LENGTH, 3 * LENGTH // 4, 1)), jnp.arange(LENGTH), side="right").astype(jnp.int32)
    targets = touch_ends(skewed_ids(own_keys[2], (LENGTH,), VOCAB, 2), jax.random.fold_in(own_keys[2], 3), 0, VOCAB - 1).astype(jnp.int32)
    loss_mask = draw_loss_mask(jax.random.fold_in(jax.random.fold_in(key_list[11], part), 71), part)
    attn_gain = jnp.clip(jnp.exp(math.log(2.0) - 1.3862944 * jax.random.uniform(key_list[4], (2, D), jnp.float32) ** shard_levels(key_list[4], (2, D), ((0, 2),), -0.2, 0.2)), 0.5, 2.0)
    final_gain = jnp.clip(jnp.exp(math.log(4.0) - 1.3862944 * jax.random.uniform(key_list[5], (2, D), jnp.float32) ** shard_levels(key_list[5], (2, D), ((0, 2),), -0.2, 0.2)), 1.0, 4.0)
    w_query = draw_w_query(jax.random.fold_in(key_list[11], 71), part)
    w_key = draw_w_key(jax.random.fold_in(key_list[11], 71), part)
    w_value = normal_values(key_list[8], (2, D, KV_HEADS * HEAD_DIM), D ** -0.5, 0.09375, ((0, 2), (1, 4), (2, 2)))
    w_out = normal_values(key_list[9], (2, HEADS * HEAD_DIM, D), (HEADS * HEAD_DIM) ** -0.5, 0.125, ((0, 2), (1, 2), (2, 4)))
    head = draw_head(jax.random.fold_in(key_list[11], 71), part)
    return dict(hidden=hidden, segment_ids=segment_ids, targets=targets, loss_mask=loss_mask, attn_gain=attn_gain, final_gain=final_gain, w_query=w_query, w_key=w_key, w_value=w_value, w_out=w_out, head=head)


EPS = 1e-05
THETA = 500000.0

def rms_norm(values, gain):
    return values * lax.rsqrt(lax.optimization_barrier(jnp.mean(values * values, axis=-1, keepdims=True)) + EPS) * gain

def rotate(tensor, offsets):
    half = tensor.shape[-1] // 2
    freq = THETA ** (-(jnp.arange(half, dtype=jnp.float32) * 2.0 / tensor.shape[-1]))
    angle = offsets.astype(jnp.float32)[:, None] * freq[None, :]
    cosine = jnp.cos(angle)[:, None, :]
    sine = jnp.sin(angle)[:, None, :]
    first = tensor[..., :half]
    second = tensor[..., half:]
    return jnp.concatenate([first * cosine - second * sine, second * cosine + first * sine], axis=-1)

def one_model(x, gain_a, gain_f, wq, wk, wv, wo, table, segment_ids, targets, loss_mask):
    length = x.shape[0]
    position = jnp.arange(length, dtype=jnp.int32)
    labels = jnp.arange(SEGMENTS, dtype=jnp.int32)
    member = segment_ids[None, :] == labels[:, None]
    starts = lax.optimization_barrier(jnp.min(jnp.where(member, position[None, :], length), axis=1)).astype(jnp.int32)
    token_start = lax.optimization_barrier(jnp.sum(jnp.where(member, starts[:, None], 0), axis=0)).astype(jnp.int32)
    offsets = position - token_start
    xfloat = x.astype(jnp.float32)
    normed = rms_norm(xfloat, gain_a).astype(jnp.bfloat16)
    keys = jnp.dot(normed, wk, preferred_element_type=jnp.float32).reshape(length, KV_HEADS, HEAD_DIM)
    keys = rotate(keys, offsets).astype(jnp.bfloat16)
    values = jnp.dot(normed, wv, preferred_element_type=jnp.float32).reshape(length, KV_HEADS, HEAD_DIM).astype(jnp.bfloat16)
    blocks = length // TOK_DEV
    mask_blocks = loss_mask.reshape(blocks, TOK_DEV)
    ranking = jnp.cumsum(mask_blocks, axis=1) - 1
    picks = (mask_blocks[:, None, :] == 1) & (ranking[:, None, :] == jnp.arange(CAP, dtype=jnp.int32)[None, :, None])
    inside = jnp.arange(TOK_DEV, dtype=jnp.int32)
    row_pos = lax.optimization_barrier(jnp.sum(jnp.where(picks, inside[None, None, :], 0), axis=2)) + (jnp.arange(blocks, dtype=jnp.int32) * TOK_DEV)[:, None]
    row_pos = row_pos.reshape(-1).astype(jnp.int32)
    valid = jnp.any(picks, axis=2).reshape(-1)
    rows = row_pos.shape[0]
    query = jnp.dot(normed[row_pos], wq, preferred_element_type=jnp.float32).reshape(rows, HEADS, HEAD_DIM)
    query = rotate(query, offsets[row_pos]).astype(jnp.bfloat16)
    front = jnp.zeros((WINDOW, KV_HEADS, HEAD_DIM), jnp.bfloat16)
    key_pad = jnp.concatenate([front, keys], axis=0)
    value_pad = jnp.concatenate([front, values], axis=0)
    group = HEADS // KV_HEADS
    scale = HEAD_DIM ** (-0.5)

    def attend(inputs):
        qrow, where_at, begin = inputs
        kslice = lax.dynamic_slice_in_dim(key_pad, where_at + 1, WINDOW, 0)
        vslice = lax.dynamic_slice_in_dim(value_pad, where_at + 1, WINDOW, 0)
        kpos = where_at - WINDOW + 1 + jnp.arange(WINDOW, dtype=jnp.int32)
        allowed = kpos >= begin
        grouped = qrow.astype(jnp.float32).reshape(KV_HEADS, group, HEAD_DIM)
        scores = jnp.einsum('ngd,knd->ngk', grouped, kslice.astype(jnp.float32)) * scale
        scores = jnp.where(allowed[None, None, :], scores, -1e+30)
        top = lax.optimization_barrier(jnp.max(scores, axis=-1, keepdims=True))
        expo = jnp.exp(scores - top)
        weights = (expo / lax.optimization_barrier(jnp.sum(expo, axis=-1, keepdims=True))).astype(jnp.bfloat16)
        out = jnp.einsum('ngk,knd->ngd', weights.astype(jnp.float32), vslice.astype(jnp.float32))
        return out.astype(jnp.bfloat16).reshape(HEADS * HEAD_DIM)
    attended = lax.map(attend, (query, row_pos, token_start[row_pos]))
    projected = jnp.dot(attended, wo, preferred_element_type=jnp.float32)
    state = xfloat[row_pos] + projected
    final = rms_norm(state, gain_f).astype(jnp.bfloat16)
    logits = jnp.dot(final, table, preferred_element_type=jnp.float32)
    top = lax.optimization_barrier(jnp.max(logits, axis=1))
    total = lax.optimization_barrier(jnp.sum(jnp.exp(logits - top[:, None]), axis=1))
    picked = jnp.take_along_axis(logits, targets[row_pos][:, None], axis=1)[:, 0]
    result = jnp.where(valid, picked - (top + jnp.log(total)), 0.0)
    return jnp.zeros((length,), jnp.float32).at[row_pos].add(result)

def reference(hidden, segment_ids, targets, loss_mask, attn_gain, final_gain, w_query, w_key, w_value, w_out, head):
    outputs = []
    for model in range(2):
        outputs.append(one_model(hidden[model], attn_gain[model], final_gain[model], w_query[model], w_key[model], w_value[model], w_out[model], head[model], segment_ids, targets, loss_mask))
    return jnp.stack(outputs)
```

```python
import functools

import jax
import jax.numpy as jnp
import numpy as np
from jax import lax
from jax.experimental import pallas as pl
from jax.experimental.pallas import tpu as pltpu
from jax.sharding import PartitionSpec as P

HEAD_DIM = 128
WINDOW = 2048
CAP = 32
SEGMENTS = 4


EPS = 1e-05
THETA = 500000.0
FARTHEST = 1073741824


def passed_along(value, axis, by):
    length = lax.axis_size(axis)
    pairs = [(i, i + by) for i in range(length) if 0 <= i + by < length]
    return lax.ppermute(value, axis, pairs)


def joined(part, axis, combine):
    gathered = jax.tree.map(lambda a: lax.all_gather(a, axis), part)

    def take(source):
        return jax.tree.map(lambda a: lax.dynamic_index_in_dim(a, source, 0, False), gathered)

    return lax.fori_loop(
        1, lax.axis_size(axis), lambda source, state: combine(state, take(source)), take(0)
    )


def rms_norm(values, gain):
    return values * lax.rsqrt(jnp.mean(values * values, axis=-1, keepdims=True) + EPS) * gain


def rotate(tensor, offsets):
    half = tensor.shape[-1] // 2
    freq = THETA ** (-(jnp.arange(half, dtype=jnp.float32) * 2.0 / tensor.shape[-1]))
    angle = offsets.astype(jnp.float32)[:, None] * freq[None, :]
    cosine = jnp.cos(angle)[:, None, :]
    sine = jnp.sin(angle)[:, None, :]
    first = tensor[..., :half]
    second = tensor[..., half:]
    return jnp.concatenate(
        [first * cosine - second * sine, second * cosine + first * sine], axis=-1
    )


def combine_stats(left, right):
    top = jnp.maximum(left[0], right[0])
    total = left[1] * jnp.exp(left[0] - top) + right[1] * jnp.exp(right[0] - top)
    return (top, total, left[2] + right[2])


def block_stats(scores, allowed):
    row_peak = jnp.max(scores, axis=-1)
    lifted = jnp.where(allowed[None, None, :, :], jnp.exp(scores - row_peak[..., None]), 0.0)
    return (row_peak, jnp.sum(lifted, axis=-1))


def weighted_values(scores, row_peak, row_total, value_block):
    safe_total = jnp.where(row_total > 0.0, row_total, 1.0)
    weights = (jnp.exp(scores - row_peak[..., None]) / safe_total[..., None]).astype(jnp.bfloat16)
    return jnp.einsum("ngck,knd->cngd", weights, value_block, preferred_element_type=jnp.float32)


def gathered_weights(
    hidden,
    segment_ids,
    targets,
    loss_mask,
    attn_gain,
    final_gain,
    w_query,
    w_key,
    w_value,
    w_out,
    head,
):
    tokens = hidden.shape[1]
    seq_index = lax.axis_index("seq")
    base = seq_index * tokens
    position = base + jnp.arange(tokens, dtype=jnp.int32)
    whole = lax.all_gather(hidden[0], "tp", axis=1, tiled=True)
    xfloat = whole.astype(jnp.float32)
    normed = rms_norm(xfloat, attn_gain[0]).astype(jnp.bfloat16)
    labels = jnp.arange(SEGMENTS, dtype=jnp.int32)
    member = segment_ids[None, :] == labels[:, None]
    local_first = jnp.min(jnp.where(member, position[None, :], FARTHEST), axis=1)
    starts = lax.pmin(local_first, "seq")
    token_start = jnp.sum(jnp.where(member, starts[:, None], 0), axis=0)
    offsets = position - token_start
    ranking = jnp.cumsum(loss_mask) - 1
    picks = (loss_mask[None, :] == 1) & (
        ranking[None, :] == jnp.arange(CAP, dtype=jnp.int32)[:, None]
    )
    chooser = picks.astype(jnp.bfloat16)
    normed_rows = jnp.dot(chooser, normed, preferred_element_type=jnp.float32).astype(jnp.bfloat16)
    x_rows = jnp.dot(chooser, whole, preferred_element_type=jnp.float32)
    row_pos = jnp.sum(jnp.where(picks, position[None, :], 0), axis=1)
    row_start = jnp.sum(jnp.where(picks, token_start[None, :], 0), axis=1)
    row_target = jnp.sum(jnp.where(picks, targets[None, :], 0), axis=1)
    places = jnp.stack([row_pos, row_start])
    query_cols = w_query.shape[2]
    key_cols = w_key.shape[2]
    local_heads = query_cols // HEAD_DIM
    local_kv = key_cols // HEAD_DIM
    group = local_heads // local_kv
    score_scale = HEAD_DIM ** (-0.5)
    query = jnp.dot(
        normed_rows,
        lax.all_gather(w_query[0], "seq", axis=0, tiled=True),
        preferred_element_type=jnp.float32,
    )
    keys = jnp.dot(
        normed,
        lax.all_gather(w_key[0], "seq", axis=0, tiled=True),
        preferred_element_type=jnp.float32,
    )
    values = jnp.dot(
        normed,
        lax.all_gather(w_value[0], "seq", axis=0, tiled=True),
        preferred_element_type=jnp.float32,
    )
    query = rotate(query.reshape(CAP, local_heads, HEAD_DIM), row_pos - row_start).astype(
        jnp.bfloat16
    )
    keys = rotate(keys.reshape(tokens, local_kv, HEAD_DIM), offsets).astype(jnp.bfloat16)
    values = values.reshape(tokens, local_kv, HEAD_DIM).astype(jnp.bfloat16)

    def masked_scores(query_rows, bounds, key_block, key_base):
        key_pos = key_base + jnp.arange(key_block.shape[0], dtype=jnp.int32)
        row_at = bounds[0][:, None]
        allowed = (key_pos[None, :] <= row_at) & (row_at - key_pos[None, :] < WINDOW)
        allowed = allowed & (key_pos[None, :] >= bounds[1][:, None])
        grouped = query_rows.reshape(CAP, local_kv, group, HEAD_DIM)
        scores = (
            jnp.einsum("cngd,knd->ngck", grouped, key_block, preferred_element_type=jnp.float32)
            * score_scale
        )
        return (jnp.where(allowed[None, None, :, :], scores, -1e30), allowed)

    reach = min(WINDOW // tokens, lax.axis_size("seq") - 1)
    own_scores, own_allowed = masked_scores(query, places, keys, base)
    row_peak, row_total = block_stats(own_scores, own_allowed)
    visited = []
    for step in range(1, reach + 1):
        guest = passed_along(query, "seq", -step)
        guest_places = passed_along(places, "seq", -step)
        guest_scores, guest_allowed = masked_scores(guest, guest_places, keys, base)
        guest_peak, guest_total = block_stats(guest_scores, guest_allowed)
        returned = passed_along(jnp.stack([guest_peak, guest_total]), "seq", step)
        back_peak = jnp.where(seq_index >= step, returned[0], -1e30)
        merged_peak = jnp.maximum(row_peak, back_peak)
        row_total = row_total * jnp.exp(row_peak - merged_peak) + returned[1] * jnp.exp(
            back_peak - merged_peak
        )
        row_peak = merged_peak
        visited.append(guest_scores)
    attended = weighted_values(own_scores, row_peak, row_total, values)
    for step in range(1, reach + 1):
        guest_stats = passed_along(jnp.stack([row_peak, row_total]), "seq", -step)
        share = weighted_values(visited[step - 1], guest_stats[0], guest_stats[1], values)
        attended = attended + passed_along(share, "seq", step)
    attended = attended.astype(jnp.bfloat16).reshape(CAP, query_cols)
    partial_out = jnp.dot(
        attended,
        lax.all_gather(w_out[0], "seq", axis=1, tiled=True),
        preferred_element_type=jnp.float32,
    )
    summed = lax.psum(partial_out, "tp")
    state = x_rows + summed
    final = rms_norm(state, final_gain[0]).astype(jnp.bfloat16)
    all_rows = lax.all_gather(final, "seq", axis=0, tiled=True)
    all_targets = lax.all_gather(row_target, "seq", axis=0, tiled=True)
    logits = jnp.dot(all_rows, head[0], preferred_element_type=jnp.float32)
    vocab_start = (seq_index * lax.axis_size("tp") + lax.axis_index("tp")) * head.shape[2]
    local_top = jnp.max(logits, axis=1)
    local_total = jnp.sum(jnp.exp(logits - local_top[:, None]), axis=1)
    hit = all_targets[:, None] == vocab_start + jnp.arange(head.shape[2], dtype=jnp.int32)[None, :]
    local_target = jnp.sum(jnp.where(hit, logits, 0.0), axis=1)
    merged_top, merged_total, merged_target = joined(
        (local_top, local_total, local_target), ("seq", "tp"), combine_stats
    )
    logp = merged_target - (merged_top + jnp.log(merged_total))
    own = lax.dynamic_slice_in_dim(logp, seq_index * CAP, CAP, 0)
    placed = jnp.sum(jnp.where(picks, own[:, None], 0.0), axis=0)
    return placed[None, :].astype(jnp.float32)


def place():
    return lax.axis_index("seq"), lax.axis_index("tp")


def greet(peers):
    barrier = pltpu.get_barrier_semaphore()
    for peer in peers:
        pl.semaphore_signal(barrier, inc=1, device_id=peer, device_id_type=pl.DeviceIdType.MESH)
    pl.semaphore_wait(barrier, len(peers))


def remote(source, target, send, recv, peer):
    return pltpu.make_async_remote_copy(
        src_ref=source,
        dst_ref=target,
        send_sem=send,
        recv_sem=recv,
        device_id=peer,
        device_id_type=pl.DeviceIdType.MESH,
    )


def everyone(seq, tp):
    s, t = place()
    return [
        ((d, e), {"seq": lax.rem(s + d, seq), "tp": lax.rem(t + e, tp)})
        for d in range(seq)
        for e in range(tp)
        if (d, e) != (0, 0)
    ]


def tell_all(seq, tp, value, out, send, recv):
    s, t = place()
    out[s, t] = value[...]
    copies = []
    for number, (_, peer) in enumerate(everyone(seq, tp)):
        copy = remote(value, out.at[s, t], send.at[number], recv.at[number], peer)
        copy.start()
        copies.append(copy)
    return copies


def fused_kernel(
    seq,
    x,
    segs,
    mask,
    target_ids,
    freq,
    attn_gain,
    final_gain,
    wq_hbm,
    wk_hbm,
    wv_hbm,
    wo_hbm,
    head_hbm,
    out,
    wq,
    wk,
    wv,
    wo,
    head,
    meta,
    told,
    half,
    blocks,
    parts,
    inbox,
    qparts,
    qinbox,
    picks,
    rowinfo,
    scales,
    tables,
    keys,
    values,
    queries,
    att,
    rawrows,
    away,
    arrived_away,
    here,
    fin,
    logits,
    squares,
    sqtold,
    stats,
    sttold,
    wsem,
    xsend,
    xrecv,
    send,
    recv,
    fsend,
    frecv,
    msend,
    mrecv,
    csend,
    crecv,
    qsend,
    qrecv,
    asend,
    arecv,
    esend,
    erecv,
    zsend,
    zrecv,
    bsend,
    brecv,
    sqsend,
    sqrecv,
    stsend,
    strecv,
):
    f32, bf16 = jnp.float32, jnp.bfloat16
    s, t = place()
    other = 1 - t
    side = s // 2
    is_end = jnp.logical_or(s == 0, s == seq - 1)
    is_mid = jnp.logical_not(is_end)
    home = side == t
    tokens = x.shape[0]
    model = x.shape[1] * 2
    rows = tokens // 4
    width = model // seq
    beside = {"seq": s, "tp": other}
    dot = functools.partial(jnp.dot, preferred_element_type=f32)

    loads = [
        pltpu.make_async_copy(a, b, wsem.at[i])
        for i, (a, b) in enumerate(
            ((wk_hbm, wk), (wv_hbm, wv), (wq_hbm, wq), (wo_hbm, wo), (head_hbm, head))
        )
    ]
    for load in loads:
        load.start()
    greet([peer for _, peer in everyone(seq, 2)])

    def piece(which, p, i):
        at = pl.multiple_of((which * 2 + p) * rows, rows)
        return x.at[pl.ds(at, rows), pl.ds(i * width, width)]

    def got(p, i):
        return half.at[p, :, pl.ds(i * width, width)]

    pairs = [(p, i) for p in range(2) for i in range(2)]
    firsts = {
        (p, i): remote(piece(other, p, i), got(p, i), xsend.at[p, i], xrecv.at[p, i], beside)
        for p, i in pairs
    }
    for pair in pairs:
        firsts[pair].start()

    def arrived(source, p):
        block = blocks.at[source, t * 2 + p]
        return remote(block, block, send.at[source, p], recv.at[source, p], beside)

    def passed(source, p):
        block = blocks.at[source, t * 2 + p]
        return remote(block, block, fsend.at[source, p], frecv.at[source, p], beside)

    def hand(view, target, p):
        remote(
            view, blocks.at[s, t * 2 + p], send.at[target, p], recv.at[s, p], {"seq": target, "tp": t}
        ).start()

    for p, i in pairs:
        target = t * 2 + i

        @pl.when(target != s)
        def _():
            hand(piece(t, p, i), target, p)

        @pl.when(target == s)
        def _():
            remote(
                piece(t, p, i), blocks.at[s, t * 2 + p], fsend.at[s, p], frecv.at[s, p], beside
            ).start()
            blocks[s, t * 2 + p] = piece(t, p, i)[...]
            blocks[s, other * 2 + p] = piece(other, p, i)[...]

    fold = jnp.zeros((tokens, 128), f32)
    for c in range(x.shape[1] // 128):
        part = x[:, c * 128 : (c + 1) * 128].astype(f32)
        fold = fold + part * part
    meta[0:1, :] = segs[...].astype(f32)
    meta[1:2, :] = mask[...].astype(f32)
    meta[2:3, :] = target_ids[...].astype(f32)
    meta[3:4, :] = jnp.sum(fold.T, axis=0, keepdims=True)
    meta[4:8, :] = jnp.zeros((4, tokens), f32)
    messages = tell_all(seq, 2, meta, told, msend, mrecv)

    for p, i in pairs:
        firsts[p, i].wait_recv()
        target = other * 2 + i

        @pl.when(target != s)
        def _():
            hand(got(p, i), target, p)

        @pl.when(target == s)
        def _():
            blocks[s, t * 2 + p] = got(p, i)[...]

    for message in messages:
        message.wait_recv()

    upper = lax.broadcasted_iota(jnp.int32, (tokens, tokens), 0)
    upper = (upper <= lax.broadcasted_iota(jnp.int32, (tokens, tokens), 1)).astype(f32).astype(bf16)
    spot = lax.broadcasted_iota(jnp.int32, (1, tokens), 1).astype(f32)
    order = lax.broadcasted_iota(jnp.int32, (CAP, tokens), 0).astype(f32) + 1.0
    begins = [jnp.full((1, 1), float(FARTHEST), f32) for _ in range(SEGMENTS)]
    for b in range(seq):
        seg = told[b, 0, 0:1, :]
        for j in range(SEGMENTS):
            low = jnp.where(seg == float(j), spot + float(b * tokens), float(FARTHEST))
            begins[j] = jnp.minimum(begins[j], jnp.min(low, axis=1, keepdims=True))
    for b in range(seq):
        chosen = told[b, 0, 1:2, :]
        rank = dot(jnp.broadcast_to(chosen, (8, tokens)).astype(bf16), upper)[0:1, :]
        hit = jnp.logical_and(chosen == 1.0, rank == order)
        picks[b] = jnp.where(hit, 1.0, 0.0).astype(bf16)

        def column(line):
            return jnp.sum(jnp.where(hit, line, 0.0), axis=1, keepdims=True)

        scale = lax.rsqrt((told[b, 0, 3:4, :] + told[b, 1, 3:4, :]) / model + EPS)
        scales[0:1, b * tokens : (b + 1) * tokens] = scale
        seg = column(told[b, 0, 0:1, :])
        begin = jnp.zeros((CAP, 1), f32)
        for j in range(SEGMENTS):
            begin = begin + jnp.where(seg == float(j), begins[j], 0.0)
        here_rows = slice(b * CAP, (b + 1) * CAP)
        info = (column(spot + float(b * tokens)), begin, column(told[b, 0, 2:3, :]), column(scale))
        for kind, value in enumerate(info):
            rowinfo[kind, here_rows] = jnp.broadcast_to(value, (CAP, 128))

    gain = attn_gain[0:1, pl.ds(pl.multiple_of(s * width, width), width)]
    for load in loads[:3]:
        load.wait()
    kcols = wk.shape[1] // 2
    qcols = wq.shape[1] // 2
    partner = s + 1 - 2 * lax.rem(s, 2)
    near, far = 2 - side, 3 * (1 - side)

    def choose(number, options):
        value = options[-1]
        for k in range(len(options) - 2, -1, -1):
            value = jnp.where(number == k, options[k], value)
        return value

    def pick_from(number, codes):
        code = choose(number, codes)
        return choose(code // 4, (s, partner, near, far)), jnp.where(
            lax.rem(code, 4) < 2, t * 2 + lax.rem(code, 4), other * 2 + lax.rem(code, 4) - 2
        ), lax.rem(code, 4)

    def tok_ship(d, source, g):
        peer = {"seq": lax.rem(s + 2 * d - 1 + seq, seq), "tp": t}
        chunk = source * 4 + g
        return remote(
            parts.at[d, chunk], inbox.at[d, chunk], csend.at[d, chunk], crecv.at[d, chunk], peer
        )

    def que_ship(d, source):
        peer = {"seq": lax.rem(s + 2 * d - 1 + seq, seq), "tp": t}
        return remote(
            qparts.at[d, source], qinbox.at[d, source], qsend.at[d, source], qrecv.at[d, source], peer
        )

    def ship(d, source, g, last):
        tok_ship(d, source, g).start()

        @pl.when(last)
        def _():
            que_ship(d, source).start()

    def await_ship(d, source, g, last):
        tok_ship(d, source, g).wait_recv()

        @pl.when(last)
        def _():
            que_ship(d, source).wait_recv()

    def project(source, g, last):
        block = (blocks[source, g].astype(f32) * gain).astype(bf16)
        chunk = source * 4 + g
        for d in range(2):
            cols = slice(d * kcols, (d + 1) * kcols)
            parts[d, chunk, :, :kcols] = dot(block, wk[:, cols]).astype(bf16)
            parts[d, chunk, :, kcols:] = dot(block, wv[:, cols]).astype(bf16)

        @pl.when(last)
        def _():
            raw = dot(picks[source], blocks[source].reshape(tokens, width))
            rawrows[source] = raw.astype(bf16)
            taken = (raw * gain).astype(bf16)
            for d in range(2):
                cols = slice(d * qcols, (d + 1) * qcols)
                qparts[d, source] = dot(taken, wq[:, cols]).astype(bf16)

        @pl.when(is_end)
        def _():
            ship(1 - side, source, g, last)

    def combine(d, source, g, last):
        await_ship(d, source, g, last)
        chunk = source * 4 + g
        both = parts[d, chunk].astype(f32) + inbox[d, chunk].astype(f32)
        parts[d, chunk] = both.astype(bf16)

        @pl.when(last)
        def _():
            both = qparts[d, source].astype(f32) + qinbox[d, source].astype(f32)
            qparts[d, source] = both.astype(bf16)

        ship(d, source, g, last)

    chunks = 4 * seq
    order_own = (0, 1, 4, 5, 2, 3, 8, 12, 6, 7, 9, 13, 10, 14, 11, 15)
    order_one = (4, 0, 5, 1, 8, 12, 6, 2, 7, 3, 9, 13, 10, 14, 11, 15)
    order_two = (12, 8, 0, 4, 9, 13, 10, 14, 11, 15, 1, 5, 2, 6, 3, 7)
    order_end = (12, 8, 4, 0, 9, 13, 10, 14, 11, 15, 5, 1, 6, 2, 7, 3)
    lag_one, lag_two = 4, 8

    def step(number, carry):
        @pl.when(number < chunks)
        def _():
            source, g, kind = pick_from(number, order_own)

            @pl.when(jnp.logical_and(kind < 2, source != s))
            def _():
                arrived(source, kind).wait_recv()
                passed(source, kind).start()

            awaits = jnp.logical_not(jnp.logical_and(source == s, home))

            @pl.when(jnp.logical_and(kind >= 2, awaits))
            def _():
                passed(source, kind - 2).wait_recv()

            project(source, g, kind == 3)

        one = number - lag_one

        @pl.when(jnp.logical_and(is_mid, jnp.logical_and(one >= 0, one < chunks)))
        def _():
            source, g, kind = pick_from(one, order_one)
            combine(1 - side, source, g, kind == 3)

        two = number - lag_two

        @pl.when(jnp.logical_and(is_mid, jnp.logical_and(two >= 0, two < chunks)))
        def _():
            source, g, kind = pick_from(two, order_two)
            combine(side, source, g, kind == 3)

        return carry

    lax.fori_loop(0, chunks + lag_two, step, 0)

    def turned(values, cosine, sine):
        return values * cosine + pltpu.roll(values, HEAD_DIM // 2, 1) * sine

    per = seq // 2

    def tell(b, hop):
        peer = {"seq": s + hop * (1 - 2 * side), "tp": t}
        block = att.at[side, b]
        return remote(block, block, asend.at[b, hop], arecv.at[side, b], peer)

    def told_of(source_side, b):
        block = att.at[source_side, b]
        return remote(block, block, asend.at[b, 0], arecv.at[source_side, b], beside)

    def cross(i):
        return remote(away.at[i], arrived_away.at[i], esend.at[i], erecv.at[i], beside)

    length = seq * tokens
    sign = jnp.where(lax.broadcasted_iota(jnp.int32, (1, HEAD_DIM), 1) < HEAD_DIM // 2, -1.0, 1.0)
    kv = kcols // HEAD_DIM
    group = qcols // kcols

    @pl.when(is_end)
    def _():
        def table(b, carry):
            at = pl.ds(pl.multiple_of(b * rows, rows), rows)
            line = lax.broadcasted_iota(jnp.int32, (rows, HEAD_DIM), 0) + b * rows
            angle = line.astype(f32) * freq[...]
            tables[0, at] = jnp.cos(angle)
            tables[1, at] = jnp.sin(angle) * sign
            return carry

        lax.fori_loop(0, length // rows, table, 0)
        angle = rowinfo[0] * freq[...]
        tables[0, length:] = jnp.cos(angle)
        tables[1, length:] = jnp.sin(angle) * sign

        def settle(number, carry):
            source, g, kind = pick_from(number, order_end)
            await_ship(side, source, g, kind == 3)
            chunk = source * 4 + g
            both = parts[side, chunk].astype(f32) + inbox[side, chunk].astype(f32)
            at = pl.ds(pl.multiple_of(chunk * rows, rows), rows)
            cosine, sine = tables[0, at], tables[1, at]
            for j in range(kv):
                key = both[:, j * HEAD_DIM : (j + 1) * HEAD_DIM]
                keys[j, at] = turned(key, cosine, sine).astype(bf16)
                values[j, at] = both[:, kcols + j * HEAD_DIM : kcols + (j + 1) * HEAD_DIM].astype(bf16)

            @pl.when(kind == 3)
            def _():
                both = qparts[side, source].astype(f32) + qinbox[side, source].astype(f32)
                at = pl.ds(pl.multiple_of(source * CAP, CAP), CAP)
                far_at = pl.ds(pl.multiple_of(length + source * CAP, CAP), CAP)
                cosine, sine = tables[0, far_at], tables[1, far_at]
                both = both * rowinfo[3, at][:, 0:1]
                for j in range(kv * group):
                    query = both[:, j * HEAD_DIM : (j + 1) * HEAD_DIM]
                    queries[j, at] = turned(query, cosine, sine).astype(bf16)

            return carry

        lax.fori_loop(0, chunks, settle, 0)
        position = lax.broadcasted_iota(jnp.int32, (1, length), 1).astype(f32)
        scale = scales[0:1, :]
        for which in (other, t):
            at = pl.ds(pl.multiple_of(which * per * CAP, per * CAP), per * CAP)
            row_at, row_start = rowinfo[0, at][:, 0:1], rowinfo[1, at][:, 0:1]
            allowed = jnp.logical_and(position <= row_at, position >= row_start)
            allowed = jnp.logical_and(allowed, row_at - position < float(WINDOW))
            for j in range(kv * group):
                scores = lax.dot_general(
                    queries[j, at], keys[j // group], (((1,), (1,)), ((), ())), preferred_element_type=f32
                )
                scores = jnp.where(allowed, scores * (scale * HEAD_DIM ** (-0.5)), -1e30)
                lifted = jnp.exp(scores - jnp.max(scores, axis=1, keepdims=True))
                lifted = lifted * (1.0 / jnp.sum(lifted, axis=1, keepdims=True))
                result = dot((lifted * scale).astype(bf16), values[j // group]).astype(bf16)
                for b in range(per):
                    cols = slice(j * HEAD_DIM, (j + 1) * HEAD_DIM)
                    att[side, which * per + b, :, cols] = result[b * CAP : (b + 1) * CAP]
            for b in range(per):
                for hop in range(seq - 1, 0, -1):
                    tell(which * per + b, hop).start()

    loads[3].wait()
    late_gain = final_gain[0:1, pl.ds(pl.multiple_of(s * width, width), width)]
    turns = [other * per, other * per + 1, t * per, t * per + 1]
    for k, b in enumerate(turns):
        for source_side in range(2):

            @pl.when(s != (seq - 1) * source_side)
            def _():
                told_of(source_side, b).wait_recv()

        result = dot(att[0, b], wo[:qcols]) + dot(att[1, b], wo[qcols:])
        if k < per:
            away[k] = result.astype(bf16)
            cross(k).start()
        else:
            here[k - per] = result + rawrows[b].astype(f32)

    def along(source, target, i):
        block = fin.at[source, t, i]
        return remote(
            block, block, zsend.at[i, target], zrecv.at[source, i], {"seq": target, "tp": t}
        )

    def across(source, i):
        return remote(
            fin.at[source, t, i], fin.at[source, t, i], bsend.at[source, i], brecv.at[source, i], beside
        )

    fold = []
    for i in range(per):
        cross(i).wait_recv()
        state = here[i] + arrived_away[i].astype(f32)
        fin[s, t, i] = (state * late_gain).astype(bf16)
        across(s, i).start()
        for hop in range(1, seq):
            for d in range(2):
                target = s + hop * (2 * d - 1)

                @pl.when(jnp.logical_and(target >= 0, target < seq))
                def _():
                    along(s, target, i).start()

        total = jnp.zeros((CAP, 128), f32)
        for c in range(width // 128):
            part = state[:, c * 128 : (c + 1) * 128]
            total = total + part * part
        fold.append(total)
    zero = jnp.zeros((CAP, 128), f32)
    lower = t == 0
    fold = [jnp.where(lower, v, zero) for v in fold] + [jnp.where(lower, zero, v) for v in fold]
    total = jnp.concatenate(fold, axis=0)
    squares[...] = jnp.broadcast_to(jnp.sum(total.T, axis=0, keepdims=True), squares.shape)
    sqmessages = tell_all(seq, 2, squares, sqtold, sqsend, sqrecv)
    loads[4].wait()

    def add(source, which, i, fresh):
        at = pl.ds(pl.multiple_of((which * per + i) * CAP, CAP), CAP)
        weight = head[pl.ds(pl.multiple_of(source * width, width), width)]
        value = dot(fin[source, which, i], weight)
        logits[at] = value if fresh else logits[at] + value

    for i in range(per):
        add(s, t, i, True)
    for i in range(per):
        across(s, i).wait_recv()
        add(s, other, i, True)
    for hop in range(1, seq):
        for d in range(2):
            source = s - hop * (2 * d - 1)

            @pl.when(jnp.logical_and(source >= 0, source < seq))
            def _():
                for i in range(per):
                    along(source, s, i).wait_recv()
                    across(source, i).start()
                    add(source, t, i, False)

        for d in range(2):
            source = s - hop * (2 * d - 1)

            @pl.when(jnp.logical_and(source >= 0, source < seq))
            def _():
                for i in range(per):
                    across(source, i).wait_recv()
                    add(source, other, i, False)

    for message in sqmessages:
        message.wait_recv()
    total = jnp.zeros(squares.shape, f32)
    for b in range(seq):
        total = total + sqtold[b, 0] + sqtold[b, 1]
    count = seq * CAP
    mean = jnp.broadcast_to(total[0:1, :], (count, count)).T[:, 0:1] / model
    final = logits[...] * lax.rsqrt(mean + EPS)
    entries = final.shape[1]
    top = jnp.max(final, axis=1, keepdims=True)
    exps = jnp.sum(jnp.exp(final - top), axis=1, keepdims=True)
    label = lax.broadcasted_iota(jnp.int32, (1, entries), 1) + (s * 2 + t) * entries
    found = jnp.sum(
        jnp.where(rowinfo[2][:, 0:1] == label.astype(f32), final, 0.0), axis=1, keepdims=True
    )
    lane = lax.broadcasted_iota(jnp.int32, (count, count), 1)
    packed = jnp.where(lane == 0, top, jnp.where(lane == 1, exps, jnp.where(lane == 2, found, 0.0)))
    stats[...] = packed.T[0:8, :]
    stmessages = tell_all(seq, 2, stats, sttold, stsend, strecv)
    for message in stmessages:
        message.wait_recv()
    everyones = [sttold[b, e] for b in range(seq) for e in range(2)]
    best = everyones[0][0:1, :]
    for value in everyones[1:]:
        best = jnp.maximum(best, value[0:1, :])
    summed = jnp.zeros((1, count), f32)
    hits = jnp.zeros((1, count), f32)
    for value in everyones:
        summed = summed + value[1:2, :] * jnp.exp(value[0:1, :] - best)
        hits = hits + value[2:3, :]
    logp = hits - (best + jnp.log(summed))
    own = picks[s].astype(f32)
    select = jnp.concatenate([jnp.where(s == b, own, 0.0) for b in range(seq)], axis=0)
    column = jnp.broadcast_to(logp, (count, count)).T[:, 0:1]
    out[...] = jnp.sum(select * column, axis=0, keepdims=True)

    for pair in pairs:
        firsts[pair].wait_send()
    for source in range(seq):
        for p in range(2):

            @pl.when(source != s)
            def _():
                arrived(source, p).wait_send()

            @pl.when(jnp.logical_or(source != s, home))
            def _():
                passed(source, p).wait_send()

    for message in messages + sqmessages + stmessages:
        message.wait_send()
    for d in range(2):

        @pl.when(s != (seq - 1) * d)
        def _():
            for source in range(seq):
                for g in range(4):
                    tok_ship(d, source, g).wait_send()
                que_ship(d, source).wait_send()

    @pl.when(is_end)
    def _():
        for b in range(seq):
            for hop in range(1, seq):
                tell(b, hop).wait_send()

    for i in range(per):
        cross(i).wait_send()
        for source in range(seq):
            across(source, i).wait_send()

            @pl.when(source != s)
            def _():
                along(s, source, i).wait_send()


def fused_rows(
    hidden,
    segment_ids,
    targets,
    loss_mask,
    attn_gain,
    final_gain,
    w_query,
    w_key,
    w_value,
    w_out,
    head,
):
    seq = lax.axis_size("seq")
    tokens, features = hidden.shape[1:]
    model = features * 2
    width = w_key.shape[1]
    rows = tokens // 4
    kcols = w_key.shape[2] // 2
    qcols = w_query.shape[2] // 2
    kv = kcols // HEAD_DIM
    entries = head.shape[2]
    count = seq * CAP
    freq = THETA ** (-(np.arange(HEAD_DIM // 2) * 2.0 / HEAD_DIM))
    freq = jnp.asarray(np.concatenate([freq, freq])[None, :].astype(np.float32))
    vmem = pl.BlockSpec(memory_space=pltpu.VMEM)
    hbm = pl.BlockSpec(memory_space=pl.ANY)
    bf16, f32 = jnp.bfloat16, jnp.float32
    dma = pltpu.SemaphoreType.DMA
    return pl.pallas_call(
        functools.partial(fused_kernel, seq),
        out_shape=jax.ShapeDtypeStruct((1, tokens), f32),
        in_specs=[vmem] * 7 + [hbm] * 5,
        out_specs=vmem,
        scratch_shapes=[
            pltpu.VMEM(w_query.shape[1:], bf16),
            pltpu.VMEM(w_key.shape[1:], bf16),
            pltpu.VMEM(w_value.shape[1:], bf16),
            pltpu.VMEM(w_out.shape[1:], bf16),
            pltpu.VMEM(head.shape[1:], bf16),
            pltpu.VMEM((8, tokens), f32),
            pltpu.VMEM((seq, 2, 8, tokens), f32),
            pltpu.VMEM((2, rows, features), bf16),
            pltpu.VMEM((seq, 4, rows, width), bf16),
            pltpu.VMEM((2, 4 * seq, rows, 2 * kcols), bf16),
            pltpu.VMEM((2, 4 * seq, rows, 2 * kcols), bf16),
            pltpu.VMEM((2, seq, CAP, qcols), bf16),
            pltpu.VMEM((2, seq, CAP, qcols), bf16),
            pltpu.VMEM((seq, CAP, tokens), bf16),
            pltpu.VMEM((4, count, 128), f32),
            pltpu.VMEM((8, seq * tokens), f32),
            pltpu.VMEM((2, seq * tokens + count, HEAD_DIM), f32),
            pltpu.VMEM((kv, seq * tokens, HEAD_DIM), bf16),
            pltpu.VMEM((kv, seq * tokens, HEAD_DIM), bf16),
            pltpu.VMEM((qcols // HEAD_DIM, count, HEAD_DIM), bf16),
            pltpu.VMEM((2, seq, CAP, qcols), bf16),
            pltpu.VMEM((seq, CAP, width), bf16),
            pltpu.VMEM((seq // 2, CAP, width), bf16),
            pltpu.VMEM((seq // 2, CAP, width), bf16),
            pltpu.VMEM((seq // 2, CAP, width), f32),
            pltpu.VMEM((seq, 2, seq // 2, CAP, width), bf16),
            pltpu.VMEM((count, entries), f32),
            pltpu.VMEM((8, count), f32),
            pltpu.VMEM((seq, 2, 8, count), f32),
            pltpu.VMEM((8, count), f32),
            pltpu.VMEM((seq, 2, 8, count), f32),
            dma((5,)),
            dma((2, 2)),
            dma((2, 2)),
            dma((seq, 2)),
            dma((seq, 2)),
            dma((seq, 2)),
            dma((seq, 2)),
            dma((2 * seq,)),
            dma((2 * seq,)),
            dma((2, 4 * seq)),
            dma((2, 4 * seq)),
            dma((2, seq)),
            dma((2, seq)),
            dma((seq, seq)),
            dma((2, seq)),
            dma((seq // 2,)),
            dma((seq // 2,)),
            dma((seq // 2, seq)),
            dma((seq, seq // 2)),
            dma((seq, seq // 2)),
            dma((seq, seq // 2)),
            dma((2 * seq,)),
            dma((2 * seq,)),
            dma((2 * seq,)),
            dma((2 * seq,)),
        ],
        compiler_params=pltpu.CompilerParams(collective_id=0, has_side_effects=True),
    )(
        hidden[0],
        segment_ids[None, :],
        loss_mask[None, :],
        targets[None, :],
        freq,
        attn_gain,
        final_gain,
        w_query[0],
        w_key[0],
        w_value[0],
        w_out[0],
        head[0],
    )


def solution(mesh):
    placed = (
        P("ref", ("groups", "seq"), "tp"),
        P(("groups", "seq")),
        P(("groups", "seq")),
        P(("groups", "seq")),
        P("ref", None),
        P("ref", None),
        P("ref", "seq", "tp"),
        P("ref", "seq", "tp"),
        P("ref", "seq", "tp"),
        P("ref", "tp", "seq"),
        P("ref", None, ("seq", "tp")),
    )

    def shards(*args):
        seq, tp = mesh.shape["seq"], mesh.shape["tp"]
        own_heads = args[7].shape[2] // HEAD_DIM
        moves = tp == 2 and seq == 4 and own_heads == seq and args[6].shape[2] == 2 * args[7].shape[2]
        return (fused_rows if moves else gathered_weights)(*args)

    return jax.shard_map(
        shards, mesh=mesh, in_specs=placed, out_specs=P("ref", ("groups", "seq")), check_vma=False
    )
```

```python
import functools

import jax
import jax.numpy as jnp
import numpy as np
from jax import lax
from jax.experimental import pallas as pl
from jax.experimental.pallas import tpu as pltpu
from jax.sharding import PartitionSpec as P

HEAD_DIM = 128
WINDOW = 2048
CAP = 32
SEGMENTS = 4


EPS = 1e-05
THETA = 500000.0
FARTHEST = 1073741824


def passed_along(value, axis, by):
    length = lax.axis_size(axis)
    pairs = [(i, i + by) for i in range(length) if 0 <= i + by < length]
    return lax.ppermute(value, axis, pairs)


def joined(part, axis, combine):
    gathered = jax.tree.map(lambda a: lax.all_gather(a, axis), part)

    def take(source):
        return jax.tree.map(lambda a: lax.dynamic_index_in_dim(a, source, 0, False), gathered)

    return lax.fori_loop(
        1, lax.axis_size(axis), lambda source, state: combine(state, take(source)), take(0)
    )


def rms_norm(values, gain):
    return values * lax.rsqrt(jnp.mean(values * values, axis=-1, keepdims=True) + EPS) * gain


def rotate(tensor, offsets):
    half = tensor.shape[-1] // 2
    freq = THETA ** (-(jnp.arange(half, dtype=jnp.float32) * 2.0 / tensor.shape[-1]))
    angle = offsets.astype(jnp.float32)[:, None] * freq[None, :]
    cosine = jnp.cos(angle)[:, None, :]
    sine = jnp.sin(angle)[:, None, :]
    first = tensor[..., :half]
    second = tensor[..., half:]
    return jnp.concatenate(
        [first * cosine - second * sine, second * cosine + first * sine], axis=-1
    )


def combine_stats(left, right):
    top = jnp.maximum(left[0], right[0])
    total = left[1] * jnp.exp(left[0] - top) + right[1] * jnp.exp(right[0] - top)
    return (top, total, left[2] + right[2])


def block_stats(scores, allowed):
    row_peak = jnp.max(scores, axis=-1)
    lifted = jnp.where(allowed[None, None, :, :], jnp.exp(scores - row_peak[..., None]), 0.0)
    return (row_peak, jnp.sum(lifted, axis=-1))


def weighted_values(scores, row_peak, row_total, value_block):
    safe_total = jnp.where(row_total > 0.0, row_total, 1.0)
    weights = (jnp.exp(scores - row_peak[..., None]) / safe_total[..., None]).astype(jnp.bfloat16)
    return jnp.einsum("ngck,knd->cngd", weights, value_block, preferred_element_type=jnp.float32)


def gathered_weights(
    hidden,
    segment_ids,
    targets,
    loss_mask,
    attn_gain,
    final_gain,
    w_query,
    w_key,
    w_value,
    w_out,
    head,
):
    tokens = hidden.shape[1]
    seq_index = lax.axis_index("seq")
    base = seq_index * tokens
    position = base + jnp.arange(tokens, dtype=jnp.int32)
    whole = lax.all_gather(hidden[0], "tp", axis=1, tiled=True)
    xfloat = whole.astype(jnp.float32)
    normed = rms_norm(xfloat, attn_gain[0]).astype(jnp.bfloat16)
    labels = jnp.arange(SEGMENTS, dtype=jnp.int32)
    member = segment_ids[None, :] == labels[:, None]
    local_first = jnp.min(jnp.where(member, position[None, :], FARTHEST), axis=1)
    starts = lax.pmin(local_first, "seq")
    token_start = jnp.sum(jnp.where(member, starts[:, None], 0), axis=0)
    offsets = position - token_start
    ranking = jnp.cumsum(loss_mask) - 1
    picks = (loss_mask[None, :] == 1) & (
        ranking[None, :] == jnp.arange(CAP, dtype=jnp.int32)[:, None]
    )
    chooser = picks.astype(jnp.bfloat16)
    normed_rows = jnp.dot(chooser, normed, preferred_element_type=jnp.float32).astype(jnp.bfloat16)
    x_rows = jnp.dot(chooser, whole, preferred_element_type=jnp.float32)
    row_pos = jnp.sum(jnp.where(picks, position[None, :], 0), axis=1)
    row_start = jnp.sum(jnp.where(picks, token_start[None, :], 0), axis=1)
    row_target = jnp.sum(jnp.where(picks, targets[None, :], 0), axis=1)
    places = jnp.stack([row_pos, row_start])
    query_cols = w_query.shape[2]
    key_cols = w_key.shape[2]
    local_heads = query_cols // HEAD_DIM
    local_kv = key_cols // HEAD_DIM
    group = local_heads // local_kv
    score_scale = HEAD_DIM ** (-0.5)
    query = jnp.dot(
        normed_rows,
        lax.all_gather(w_query[0], "seq", axis=0, tiled=True),
        preferred_element_type=jnp.float32,
    )
    keys = jnp.dot(
        normed,
        lax.all_gather(w_key[0], "seq", axis=0, tiled=True),
        preferred_element_type=jnp.float32,
    )
    values = jnp.dot(
        normed,
        lax.all_gather(w_value[0], "seq", axis=0, tiled=True),
        preferred_element_type=jnp.float32,
    )
    query = rotate(query.reshape(CAP, local_heads, HEAD_DIM), row_pos - row_start).astype(
        jnp.bfloat16
    )
    keys = rotate(keys.reshape(tokens, local_kv, HEAD_DIM), offsets).astype(jnp.bfloat16)
    values = values.reshape(tokens, local_kv, HEAD_DIM).astype(jnp.bfloat16)

    def masked_scores(query_rows, bounds, key_block, key_base):
        key_pos = key_base + jnp.arange(key_block.shape[0], dtype=jnp.int32)
        row_at = bounds[0][:, None]
        allowed = (key_pos[None, :] <= row_at) & (row_at - key_pos[None, :] < WINDOW)
        allowed = allowed & (key_pos[None, :] >= bounds[1][:, None])
        grouped = query_rows.reshape(CAP, local_kv, group, HEAD_DIM)
        scores = (
            jnp.einsum("cngd,knd->ngck", grouped, key_block, preferred_element_type=jnp.float32)
            * score_scale
        )
        return (jnp.where(allowed[None, None, :, :], scores, -1e30), allowed)

    reach = min(WINDOW // tokens, lax.axis_size("seq") - 1)
    own_scores, own_allowed = masked_scores(query, places, keys, base)
    row_peak, row_total = block_stats(own_scores, own_allowed)
    visited = []
    for step in range(1, reach + 1):
        guest = passed_along(query, "seq", -step)
        guest_places = passed_along(places, "seq", -step)
        guest_scores, guest_allowed = masked_scores(guest, guest_places, keys, base)
        guest_peak, guest_total = block_stats(guest_scores, guest_allowed)
        returned = passed_along(jnp.stack([guest_peak, guest_total]), "seq", step)
        back_peak = jnp.where(seq_index >= step, returned[0], -1e30)
        merged_peak = jnp.maximum(row_peak, back_peak)
        row_total = row_total * jnp.exp(row_peak - merged_peak) + returned[1] * jnp.exp(
            back_peak - merged_peak
        )
        row_peak = merged_peak
        visited.append(guest_scores)
    attended = weighted_values(own_scores, row_peak, row_total, values)
    for step in range(1, reach + 1):
        guest_stats = passed_along(jnp.stack([row_peak, row_total]), "seq", -step)
        share = weighted_values(visited[step - 1], guest_stats[0], guest_stats[1], values)
        attended = attended + passed_along(share, "seq", step)
    attended = attended.astype(jnp.bfloat16).reshape(CAP, query_cols)
    partial_out = jnp.dot(
        attended,
        lax.all_gather(w_out[0], "seq", axis=1, tiled=True),
        preferred_element_type=jnp.float32,
    )
    summed = lax.psum(partial_out, "tp")
    state = x_rows + summed
    final = rms_norm(state, final_gain[0]).astype(jnp.bfloat16)
    all_rows = lax.all_gather(final, "seq", axis=0, tiled=True)
    all_targets = lax.all_gather(row_target, "seq", axis=0, tiled=True)
    logits = jnp.dot(all_rows, head[0], preferred_element_type=jnp.float32)
    vocab_start = (seq_index * lax.axis_size("tp") + lax.axis_index("tp")) * head.shape[2]
    local_top = jnp.max(logits, axis=1)
    local_total = jnp.sum(jnp.exp(logits - local_top[:, None]), axis=1)
    hit = all_targets[:, None] == vocab_start + jnp.arange(head.shape[2], dtype=jnp.int32)[None, :]
    local_target = jnp.sum(jnp.where(hit, logits, 0.0), axis=1)
    merged_top, merged_total, merged_target = joined(
        (local_top, local_total, local_target), ("seq", "tp"), combine_stats
    )
    logp = merged_target - (merged_top + jnp.log(merged_total))
    own = lax.dynamic_slice_in_dim(logp, seq_index * CAP, CAP, 0)
    placed = jnp.sum(jnp.where(picks, own[:, None], 0.0), axis=0)
    return placed[None, :].astype(jnp.float32)


def place():
    return lax.axis_index("seq"), lax.axis_index("tp")


def greet(peers):
    barrier = pltpu.get_barrier_semaphore()
    for peer in peers:
        pl.semaphore_signal(barrier, inc=1, device_id=peer, device_id_type=pl.DeviceIdType.MESH)
    pl.semaphore_wait(barrier, len(peers))


def remote(source, target, send, recv, peer):
    return pltpu.make_async_remote_copy(
        src_ref=source,
        dst_ref=target,
        send_sem=send,
        recv_sem=recv,
        device_id=peer,
        device_id_type=pl.DeviceIdType.MESH,
    )


def everyone(seq, tp):
    s, t = place()
    return [
        ((d, e), {"seq": lax.rem(s + d, seq), "tp": lax.rem(t + e, tp)})
        for d in range(seq)
        for e in range(tp)
        if (d, e) != (0, 0)
    ]


def tell_all(seq, tp, value, out, send, recv):
    s, t = place()
    out[s, t] = value[...]
    copies = []
    for number, (_, peer) in enumerate(everyone(seq, tp)):
        copy = remote(value, out.at[s, t], send.at[number], recv.at[number], peer)
        copy.start()
        copies.append(copy)
    return copies


def fused_kernel(
    seq,
    x,
    segs,
    mask,
    target_ids,
    freq,
    attn_gain,
    final_gain,
    wq_hbm,
    wk_hbm,
    wv_hbm,
    wo_hbm,
    head_hbm,
    out,
    wq,
    wk,
    wv,
    wo,
    head,
    meta,
    told,
    sums,
    sumtold,
    half,
    blocks,
    parts,
    inbox,
    qparts,
    qinbox,
    picks,
    rowinfo,
    scales,
    tables,
    keys,
    values,
    queries,
    att,
    rawrows,
    away,
    arrived_away,
    here,
    fin,
    logits,
    squares,
    sqtold,
    stats,
    sttold,
    wsem,
    xsend,
    xrecv,
    send,
    recv,
    fsend,
    frecv,
    msend,
    mrecv,
    usend,
    urecv,
    csend,
    crecv,
    qsend,
    qrecv,
    asend,
    arecv,
    esend,
    erecv,
    zsend,
    zrecv,
    bsend,
    brecv,
    sqsend,
    sqrecv,
    stsend,
    strecv,
):
    f32, bf16 = jnp.float32, jnp.bfloat16
    s, t = place()
    other = 1 - t
    side = s // 2
    is_end = jnp.logical_or(s == 0, s == seq - 1)
    is_mid = jnp.logical_not(is_end)
    home = side == t
    tokens = x.shape[0]
    model = x.shape[1] * 2
    rows = tokens // 4
    width = model // seq
    beside = {"seq": s, "tp": other}
    dot = functools.partial(jnp.dot, preferred_element_type=f32)

    loads = [
        pltpu.make_async_copy(a, b, wsem.at[i])
        for i, (a, b) in enumerate(
            ((wk_hbm, wk), (wv_hbm, wv), (wq_hbm, wq), (wo_hbm, wo), (head_hbm, head))
        )
    ]
    for load in loads:
        load.start()
    greet([peer for _, peer in everyone(seq, 2)])
    meta[0:1, :] = segs[...].astype(f32)
    meta[1:2, :] = mask[...].astype(f32)
    meta[2:3, :] = target_ids[...].astype(f32)
    meta[3:8, :] = jnp.zeros((5, tokens), f32)
    messages = tell_all(seq, 2, meta, told, msend, mrecv)

    def piece(which, p, i):
        at = pl.multiple_of((which * 2 + p) * rows, rows)
        return x.at[pl.ds(at, rows), pl.ds(i * width, width)]

    def got(p, i):
        return half.at[p, :, pl.ds(i * width, width)]

    pairs = [(p, i) for p in range(2) for i in range(2)]
    firsts = {
        (p, i): remote(piece(other, p, i), got(p, i), xsend.at[p, i], xrecv.at[p, i], beside)
        for p, i in pairs
    }
    for pair in pairs:
        firsts[pair].start()

    def arrived(source, p):
        block = blocks.at[source, t * 2 + p]
        return remote(block, block, send.at[source, p], recv.at[source, p], beside)

    def passed(source, p):
        block = blocks.at[source, t * 2 + p]
        return remote(block, block, fsend.at[source, p], frecv.at[source, p], beside)

    def hand(view, target, p):
        remote(
            view, blocks.at[s, t * 2 + p], send.at[target, p], recv.at[s, p], {"seq": target, "tp": t}
        ).start()

    for p, i in pairs:
        target = t * 2 + i

        @pl.when(target != s)
        def _():
            hand(piece(t, p, i), target, p)

        @pl.when(target == s)
        def _():
            remote(
                piece(t, p, i), blocks.at[s, t * 2 + p], fsend.at[s, p], frecv.at[s, p], beside
            ).start()
            blocks[s, t * 2 + p] = piece(t, p, i)[...]
            blocks[s, other * 2 + p] = piece(other, p, i)[...]

    fold = jnp.zeros((tokens, 128), f32)
    for c in range(x.shape[1] // 128):
        part = x[:, c * 128 : (c + 1) * 128].astype(f32)
        fold = fold + part * part
    sums[...] = jnp.broadcast_to(jnp.sum(fold.T, axis=0, keepdims=True), sums.shape)
    summessages = tell_all(seq, 2, sums, sumtold, usend, urecv)
    for p, i in pairs:
        firsts[p, i].wait_recv()
        target = other * 2 + i

        @pl.when(target != s)
        def _():
            hand(got(p, i), target, p)

        @pl.when(target == s)
        def _():
            blocks[s, t * 2 + p] = got(p, i)[...]

    for message in messages:
        message.wait_recv()

    upper = lax.broadcasted_iota(jnp.int32, (tokens, tokens), 0)
    upper = (upper <= lax.broadcasted_iota(jnp.int32, (tokens, tokens), 1)).astype(f32).astype(bf16)
    spot = lax.broadcasted_iota(jnp.int32, (1, tokens), 1).astype(f32)
    order = lax.broadcasted_iota(jnp.int32, (CAP, tokens), 0).astype(f32) + 1.0
    begins = [jnp.full((1, 1), float(FARTHEST), f32) for _ in range(SEGMENTS)]
    for b in range(seq):
        seg = told[b, 0, 0:1, :]
        for j in range(SEGMENTS):
            low = jnp.where(seg == float(j), spot + float(b * tokens), float(FARTHEST))
            begins[j] = jnp.minimum(begins[j], jnp.min(low, axis=1, keepdims=True))
    for b in range(seq):
        chosen = told[b, 0, 1:2, :]
        rank = dot(jnp.broadcast_to(chosen, (8, tokens)).astype(bf16), upper)[0:1, :]
        hit = jnp.logical_and(chosen == 1.0, rank == order)
        picks[b] = jnp.where(hit, 1.0, 0.0).astype(bf16)

        def column(line):
            return jnp.sum(jnp.where(hit, line, 0.0), axis=1, keepdims=True)

        seg = column(told[b, 0, 0:1, :])
        begin = jnp.zeros((CAP, 1), f32)
        for j in range(SEGMENTS):
            begin = begin + jnp.where(seg == float(j), begins[j], 0.0)
        here_rows = slice(b * CAP, (b + 1) * CAP)
        info = (column(spot + float(b * tokens)), begin, column(told[b, 0, 2:3, :]))
        for kind, value in enumerate(info):
            rowinfo[kind, here_rows] = jnp.broadcast_to(value, (CAP, 128))

    gain = attn_gain[0:1, pl.ds(pl.multiple_of(s * width, width), width)]
    for load in loads[:3]:
        load.wait()
    kcols = wk.shape[1] // 2
    qcols = wq.shape[1] // 2
    partner = s + 1 - 2 * lax.rem(s, 2)
    near, far = 2 - side, 3 * (1 - side)

    def choose(number, options):
        value = options[-1]
        for k in range(len(options) - 2, -1, -1):
            value = jnp.where(number == k, options[k], value)
        return value

    def pick_from(number, codes):
        code = choose(number, codes)
        return choose(code // 4, (s, partner, near, far)), jnp.where(
            lax.rem(code, 4) < 2, t * 2 + lax.rem(code, 4), other * 2 + lax.rem(code, 4) - 2
        ), lax.rem(code, 4)

    def tok_ship(d, source, g):
        peer = {"seq": lax.rem(s + 2 * d - 1 + seq, seq), "tp": t}
        chunk = source * 4 + g
        return remote(
            parts.at[d, chunk], inbox.at[d, chunk], csend.at[d, chunk], crecv.at[d, chunk], peer
        )

    def que_ship(d, source):
        peer = {"seq": lax.rem(s + 2 * d - 1 + seq, seq), "tp": t}
        return remote(
            qparts.at[d, source], qinbox.at[d, source], qsend.at[d, source], qrecv.at[d, source], peer
        )

    def ship(d, source, g, last):
        tok_ship(d, source, g).start()

        @pl.when(last)
        def _():
            que_ship(d, source).start()

    def await_ship(d, source, g, last):
        tok_ship(d, source, g).wait_recv()

        @pl.when(last)
        def _():
            que_ship(d, source).wait_recv()

    def project(source, g, last):
        block = (blocks[source, g].astype(f32) * gain).astype(bf16)
        chunk = source * 4 + g
        for d in range(2):
            cols = slice(d * kcols, (d + 1) * kcols)
            parts[d, chunk, :, :kcols] = dot(block, wk[:, cols]).astype(bf16)
            parts[d, chunk, :, kcols:] = dot(block, wv[:, cols]).astype(bf16)

        @pl.when(last)
        def _():
            raw = dot(picks[source], blocks[source].reshape(tokens, width))
            rawrows[source] = raw.astype(bf16)
            taken = (raw * gain).astype(bf16)
            for d in range(2):
                cols = slice(d * qcols, (d + 1) * qcols)
                qparts[d, source] = dot(taken, wq[:, cols]).astype(bf16)

        @pl.when(is_end)
        def _():
            ship(1 - side, source, g, last)

    def combine(d, source, g, last):
        await_ship(d, source, g, last)
        chunk = source * 4 + g
        both = parts[d, chunk].astype(f32) + inbox[d, chunk].astype(f32)
        parts[d, chunk] = both.astype(bf16)

        @pl.when(last)
        def _():
            both = qparts[d, source].astype(f32) + qinbox[d, source].astype(f32)
            qparts[d, source] = both.astype(bf16)

        ship(d, source, g, last)

    chunks = 4 * seq
    order_own = (0, 12, 1, 2, 4, 13, 3, 5, 14, 8, 6, 15, 9, 7, 10, 11)
    order_one = (12, 0, 4, 13, 1, 5, 14, 8, 2, 6, 15, 9, 3, 7, 10, 11)
    order_two = (4, 12, 5, 8, 13, 9, 6, 0, 10, 14, 7, 1, 11, 15, 2, 3)
    order_end = (0, 12, 1, 8, 13, 9, 2, 4, 10, 14, 3, 5, 11, 15, 6, 7)
    lag_one, lag_two = 4, 7

    def step(number, carry):
        @pl.when(number < chunks)
        def _():
            source, g, kind = pick_from(number, order_own)

            @pl.when(jnp.logical_and(kind < 2, source != s))
            def _():
                arrived(source, kind).wait_recv()
                passed(source, kind).start()

            awaits = jnp.logical_not(jnp.logical_and(source == s, home))

            @pl.when(jnp.logical_and(kind >= 2, awaits))
            def _():
                passed(source, kind - 2).wait_recv()

            project(source, g, kind == 3)

        one = number - lag_one

        @pl.when(jnp.logical_and(is_mid, jnp.logical_and(one >= 0, one < chunks)))
        def _():
            source, g, kind = pick_from(one, order_one)
            combine(1 - side, source, g, kind == 3)

        two = number - lag_two

        @pl.when(jnp.logical_and(is_mid, jnp.logical_and(two >= 0, two < chunks)))
        def _():
            source, g, kind = pick_from(two, order_two)
            combine(side, source, g, kind == 3)

        return carry

    lax.fori_loop(0, chunks + lag_two, step, 0)

    for message in summessages:
        message.wait_recv()
    for b in range(seq):
        scale = lax.rsqrt((sumtold[b, 0, 0:1, :] + sumtold[b, 1, 0:1, :]) / model + EPS)
        scales[0:1, b * tokens : (b + 1) * tokens] = scale
        value = jnp.sum(picks[b].astype(f32) * scale, axis=1, keepdims=True)
        rowinfo[3, b * CAP : (b + 1) * CAP] = jnp.broadcast_to(value, (CAP, 128))
    def turned(values, cosine, sine):
        return values * cosine + pltpu.roll(values, HEAD_DIM // 2, 1) * sine

    per = seq // 2

    def tell(b, hop):
        peer = {"seq": s + hop * (1 - 2 * side), "tp": t}
        block = att.at[side, b]
        return remote(block, block, asend.at[b, hop], arecv.at[side, b], peer)

    def told_of(source_side, b):
        block = att.at[source_side, b]
        return remote(block, block, asend.at[b, 0], arecv.at[source_side, b], beside)

    def cross(i):
        return remote(away.at[i], arrived_away.at[i], esend.at[i], erecv.at[i], beside)

    length = seq * tokens
    sign = jnp.where(lax.broadcasted_iota(jnp.int32, (1, HEAD_DIM), 1) < HEAD_DIM // 2, -1.0, 1.0)
    kv = kcols // HEAD_DIM
    group = qcols // kcols

    @pl.when(is_end)
    def _():
        def table(b, carry):
            at = pl.ds(pl.multiple_of(b * rows, rows), rows)
            line = lax.broadcasted_iota(jnp.int32, (rows, HEAD_DIM), 0) + b * rows
            angle = line.astype(f32) * freq[...]
            tables[0, at] = jnp.cos(angle)
            tables[1, at] = jnp.sin(angle) * sign
            return carry

        lax.fori_loop(0, length // rows, table, 0)
        angle = rowinfo[0] * freq[...]
        tables[0, length:] = jnp.cos(angle)
        tables[1, length:] = jnp.sin(angle) * sign

        def settle(number, carry):
            source, g, kind = pick_from(number, order_end)
            await_ship(side, source, g, kind == 3)
            chunk = source * 4 + g
            both = parts[side, chunk].astype(f32) + inbox[side, chunk].astype(f32)
            at = pl.ds(pl.multiple_of(chunk * rows, rows), rows)
            cosine, sine = tables[0, at], tables[1, at]
            for j in range(kv):
                key = both[:, j * HEAD_DIM : (j + 1) * HEAD_DIM]
                keys[j, at] = turned(key, cosine, sine).astype(bf16)
                values[j, at] = both[:, kcols + j * HEAD_DIM : kcols + (j + 1) * HEAD_DIM].astype(bf16)

            @pl.when(kind == 3)
            def _():
                both = qparts[side, source].astype(f32) + qinbox[side, source].astype(f32)
                at = pl.ds(pl.multiple_of(source * CAP, CAP), CAP)
                far_at = pl.ds(pl.multiple_of(length + source * CAP, CAP), CAP)
                cosine, sine = tables[0, far_at], tables[1, far_at]
                both = both * rowinfo[3, at][:, 0:1]
                for j in range(kv * group):
                    query = both[:, j * HEAD_DIM : (j + 1) * HEAD_DIM]
                    queries[j, at] = turned(query, cosine, sine).astype(bf16)

            return carry

        lax.fori_loop(0, chunks, settle, 0)
        position = lax.broadcasted_iota(jnp.int32, (1, length), 1).astype(f32)
        scale = scales[0:1, :]
        for which in (other, t):
            at = pl.ds(pl.multiple_of(which * per * CAP, per * CAP), per * CAP)
            row_at, row_start = rowinfo[0, at][:, 0:1], rowinfo[1, at][:, 0:1]
            allowed = jnp.logical_and(position <= row_at, position >= row_start)
            allowed = jnp.logical_and(allowed, row_at - position < float(WINDOW))
            for j in range(kv * group):
                scores = lax.dot_general(
                    queries[j, at], keys[j // group], (((1,), (1,)), ((), ())), preferred_element_type=f32
                )
                scores = jnp.where(allowed, scores * (scale * HEAD_DIM ** (-0.5)), -1e30)
                lifted = jnp.exp(scores - jnp.max(scores, axis=1, keepdims=True))
                lifted = lifted * (1.0 / jnp.sum(lifted, axis=1, keepdims=True))
                result = dot((lifted * scale).astype(bf16), values[j // group]).astype(bf16)
                for b in range(per):
                    cols = slice(j * HEAD_DIM, (j + 1) * HEAD_DIM)
                    att[side, which * per + b, :, cols] = result[b * CAP : (b + 1) * CAP]
            for b in range(per):
                for hop in range(seq - 1, 0, -1):
                    tell(which * per + b, hop).start()

    loads[3].wait()
    late_gain = final_gain[0:1, pl.ds(pl.multiple_of(s * width, width), width)]
    turns = [other * per, other * per + 1, t * per, t * per + 1]
    for k, b in enumerate(turns):
        for source_side in range(2):

            @pl.when(s != (seq - 1) * source_side)
            def _():
                told_of(source_side, b).wait_recv()

        result = dot(att[0, b], wo[:qcols]) + dot(att[1, b], wo[qcols:])
        if k < per:
            away[k] = result.astype(bf16)
            cross(k).start()
        else:
            here[k - per] = result + rawrows[b].astype(f32)

    def along(source, target, i):
        block = fin.at[source, t, i]
        return remote(
            block, block, zsend.at[i, target], zrecv.at[source, i], {"seq": target, "tp": t}
        )

    def across(source, i):
        return remote(
            fin.at[source, t, i], fin.at[source, t, i], bsend.at[source, i], brecv.at[source, i], beside
        )

    fold = []
    for i in range(per):
        cross(i).wait_recv()
        state = here[i] + arrived_away[i].astype(f32)
        fin[s, t, i] = (state * late_gain).astype(bf16)
        across(s, i).start()
        for hop in range(1, seq):
            for d in range(2):
                target = s + hop * (2 * d - 1)

                @pl.when(jnp.logical_and(target >= 0, target < seq))
                def _():
                    along(s, target, i).start()

        total = jnp.zeros((CAP, 128), f32)
        for c in range(width // 128):
            part = state[:, c * 128 : (c + 1) * 128]
            total = total + part * part
        fold.append(total)
    zero = jnp.zeros((CAP, 128), f32)
    lower = t == 0
    fold = [jnp.where(lower, v, zero) for v in fold] + [jnp.where(lower, zero, v) for v in fold]
    total = jnp.concatenate(fold, axis=0)
    squares[...] = jnp.broadcast_to(jnp.sum(total.T, axis=0, keepdims=True), squares.shape)
    sqmessages = tell_all(seq, 2, squares, sqtold, sqsend, sqrecv)
    loads[4].wait()

    def add(source, which, i, fresh):
        at = pl.ds(pl.multiple_of((which * per + i) * CAP, CAP), CAP)
        weight = head[pl.ds(pl.multiple_of(source * width, width), width)]
        value = dot(fin[source, which, i], weight)
        logits[at] = value if fresh else logits[at] + value

    for i in range(per):
        add(s, t, i, True)
    for i in range(per):
        across(s, i).wait_recv()
        add(s, other, i, True)
    sources = [s - hop * (2 * d - 1) for hop in range(1, seq) for d in range(2)]
    valid = [jnp.logical_and(source >= 0, source < seq) for source in sources]
    for i in range(per):
        for source, good in zip(sources, valid):

            @pl.when(good)
            def _():
                along(source, s, i).wait_recv()
                across(source, i).start()

    for source, good in zip(sources, valid):

        @pl.when(good)
        def _():
            for i in range(per):
                add(source, t, i, False)

    for source, good in zip(sources, valid):

        @pl.when(good)
        def _():
            for i in range(per):
                across(source, i).wait_recv()
                add(source, other, i, False)

    for message in sqmessages:
        message.wait_recv()
    total = jnp.zeros(squares.shape, f32)
    for b in range(seq):
        total = total + sqtold[b, 0] + sqtold[b, 1]
    count = seq * CAP
    mean = jnp.broadcast_to(total[0:1, :], (count, count)).T[:, 0:1] / model
    final = logits[...] * lax.rsqrt(mean + EPS)
    entries = final.shape[1]
    top = jnp.max(final, axis=1, keepdims=True)
    exps = jnp.sum(jnp.exp(final - top), axis=1, keepdims=True)
    label = lax.broadcasted_iota(jnp.int32, (1, entries), 1) + (s * 2 + t) * entries
    found = jnp.sum(
        jnp.where(rowinfo[2][:, 0:1] == label.astype(f32), final, 0.0), axis=1, keepdims=True
    )
    lane = lax.broadcasted_iota(jnp.int32, (count, count), 1)
    packed = jnp.where(lane == 0, top, jnp.where(lane == 1, exps, jnp.where(lane == 2, found, 0.0)))
    stats[...] = packed.T[0:8, :]
    stmessages = tell_all(seq, 2, stats, sttold, stsend, strecv)
    for message in stmessages:
        message.wait_recv()
    everyones = [sttold[b, e] for b in range(seq) for e in range(2)]
    best = everyones[0][0:1, :]
    for value in everyones[1:]:
        best = jnp.maximum(best, value[0:1, :])
    summed = jnp.zeros((1, count), f32)
    hits = jnp.zeros((1, count), f32)
    for value in everyones:
        summed = summed + value[1:2, :] * jnp.exp(value[0:1, :] - best)
        hits = hits + value[2:3, :]
    logp = hits - (best + jnp.log(summed))
    own = picks[s].astype(f32)
    select = jnp.concatenate([jnp.where(s == b, own, 0.0) for b in range(seq)], axis=0)
    column = jnp.broadcast_to(logp, (count, count)).T[:, 0:1]
    out[...] = jnp.sum(select * column, axis=0, keepdims=True)

    for pair in pairs:
        firsts[pair].wait_send()
    for source in range(seq):
        for p in range(2):

            @pl.when(source != s)
            def _():
                arrived(source, p).wait_send()

            @pl.when(jnp.logical_or(source != s, home))
            def _():
                passed(source, p).wait_send()

    for message in messages + summessages + sqmessages + stmessages:
        message.wait_send()
    for d in range(2):

        @pl.when(s != (seq - 1) * d)
        def _():
            for source in range(seq):
                for g in range(4):
                    tok_ship(d, source, g).wait_send()
                que_ship(d, source).wait_send()

    @pl.when(is_end)
    def _():
        for b in range(seq):
            for hop in range(1, seq):
                tell(b, hop).wait_send()

    for i in range(per):
        cross(i).wait_send()
        for source in range(seq):
            across(source, i).wait_send()

            @pl.when(source != s)
            def _():
                along(s, source, i).wait_send()


def fused_rows(
    hidden,
    segment_ids,
    targets,
    loss_mask,
    attn_gain,
    final_gain,
    w_query,
    w_key,
    w_value,
    w_out,
    head,
):
    seq = lax.axis_size("seq")
    tokens, features = hidden.shape[1:]
    model = features * 2
    width = w_key.shape[1]
    rows = tokens // 4
    kcols = w_key.shape[2] // 2
    qcols = w_query.shape[2] // 2
    kv = kcols // HEAD_DIM
    entries = head.shape[2]
    count = seq * CAP
    freq = THETA ** (-(np.arange(HEAD_DIM // 2) * 2.0 / HEAD_DIM))
    freq = jnp.asarray(np.concatenate([freq, freq])[None, :].astype(np.float32))
    vmem = pl.BlockSpec(memory_space=pltpu.VMEM)
    hbm = pl.BlockSpec(memory_space=pl.ANY)
    bf16, f32 = jnp.bfloat16, jnp.float32
    dma = pltpu.SemaphoreType.DMA
    return pl.pallas_call(
        functools.partial(fused_kernel, seq),
        out_shape=jax.ShapeDtypeStruct((1, tokens), f32),
        in_specs=[vmem] * 7 + [hbm] * 5,
        out_specs=vmem,
        scratch_shapes=[
            pltpu.VMEM(w_query.shape[1:], bf16),
            pltpu.VMEM(w_key.shape[1:], bf16),
            pltpu.VMEM(w_value.shape[1:], bf16),
            pltpu.VMEM(w_out.shape[1:], bf16),
            pltpu.VMEM(head.shape[1:], bf16),
            pltpu.VMEM((8, tokens), f32),
            pltpu.VMEM((seq, 2, 8, tokens), f32),
            pltpu.VMEM((8, tokens), f32),
            pltpu.VMEM((seq, 2, 8, tokens), f32),
            pltpu.VMEM((2, rows, features), bf16),
            pltpu.VMEM((seq, 4, rows, width), bf16),
            pltpu.VMEM((2, 4 * seq, rows, 2 * kcols), bf16),
            pltpu.VMEM((2, 4 * seq, rows, 2 * kcols), bf16),
            pltpu.VMEM((2, seq, CAP, qcols), bf16),
            pltpu.VMEM((2, seq, CAP, qcols), bf16),
            pltpu.VMEM((seq, CAP, tokens), bf16),
            pltpu.VMEM((4, count, 128), f32),
            pltpu.VMEM((8, seq * tokens), f32),
            pltpu.VMEM((2, seq * tokens + count, HEAD_DIM), f32),
            pltpu.VMEM((kv, seq * tokens, HEAD_DIM), bf16),
            pltpu.VMEM((kv, seq * tokens, HEAD_DIM), bf16),
            pltpu.VMEM((qcols // HEAD_DIM, count, HEAD_DIM), bf16),
            pltpu.VMEM((2, seq, CAP, qcols), bf16),
            pltpu.VMEM((seq, CAP, width), bf16),
            pltpu.VMEM((seq // 2, CAP, width), bf16),
            pltpu.VMEM((seq // 2, CAP, width), bf16),
            pltpu.VMEM((seq // 2, CAP, width), f32),
            pltpu.VMEM((seq, 2, seq // 2, CAP, width), bf16),
            pltpu.VMEM((count, entries), f32),
            pltpu.VMEM((8, count), f32),
            pltpu.VMEM((seq, 2, 8, count), f32),
            pltpu.VMEM((8, count), f32),
            pltpu.VMEM((seq, 2, 8, count), f32),
            dma((5,)),
            dma((2, 2)),
            dma((2, 2)),
            dma((seq, 2)),
            dma((seq, 2)),
            dma((seq, 2)),
            dma((seq, 2)),
            dma((2 * seq,)),
            dma((2 * seq,)),
            dma((2 * seq,)),
            dma((2 * seq,)),
            dma((2, 4 * seq)),
            dma((2, 4 * seq)),
            dma((2, seq)),
            dma((2, seq)),
            dma((seq, seq)),
            dma((2, seq)),
            dma((seq // 2,)),
            dma((seq // 2,)),
            dma((seq // 2, seq)),
            dma((seq, seq // 2)),
            dma((seq, seq // 2)),
            dma((seq, seq // 2)),
            dma((2 * seq,)),
            dma((2 * seq,)),
            dma((2 * seq,)),
            dma((2 * seq,)),
        ],
        compiler_params=pltpu.CompilerParams(collective_id=0, has_side_effects=True),
    )(
        hidden[0],
        segment_ids[None, :],
        loss_mask[None, :],
        targets[None, :],
        freq,
        attn_gain,
        final_gain,
        w_query[0],
        w_key[0],
        w_value[0],
        w_out[0],
        head[0],
    )


def solution(mesh):
    placed = (
        P("ref", ("groups", "seq"), "tp"),
        P(("groups", "seq")),
        P(("groups", "seq")),
        P(("groups", "seq")),
        P("ref", None),
        P("ref", None),
        P("ref", "seq", "tp"),
        P("ref", "seq", "tp"),
        P("ref", "seq", "tp"),
        P("ref", "tp", "seq"),
        P("ref", None, ("seq", "tp")),
    )

    def shards(*args):
        seq, tp = mesh.shape["seq"], mesh.shape["tp"]
        own_heads = args[7].shape[2] // HEAD_DIM
        moves = tp == 2 and seq == 4 and own_heads == seq and args[6].shape[2] == 2 * args[7].shape[2]
        return (fused_rows if moves else gathered_weights)(*args)

    return jax.shard_map(
        shards, mesh=mesh, in_specs=placed, out_specs=P("ref", ("groups", "seq")), check_vma=False
    )
```

```python
import functools

import jax
import jax.numpy as jnp
import numpy as np
from jax import lax
from jax.experimental import pallas as pl
from jax.experimental.pallas import tpu as pltpu
from jax.sharding import PartitionSpec as P

HEAD_DIM = 128
WINDOW = 2048
CAP = 32
SEGMENTS = 4


EPS = 1e-05
THETA = 500000.0
FARTHEST = 1073741824


def passed_along(value, axis, by):
    length = lax.axis_size(axis)
    pairs = [(i, i + by) for i in range(length) if 0 <= i + by < length]
    return lax.ppermute(value, axis, pairs)


def joined(part, axis, combine):
    gathered = jax.tree.map(lambda a: lax.all_gather(a, axis), part)

    def take(source):
        return jax.tree.map(lambda a: lax.dynamic_index_in_dim(a, source, 0, False), gathered)

    return lax.fori_loop(
        1, lax.axis_size(axis), lambda source, state: combine(state, take(source)), take(0)
    )


def rms_norm(values, gain):
    return values * lax.rsqrt(jnp.mean(values * values, axis=-1, keepdims=True) + EPS) * gain


def rotate(tensor, offsets):
    half = tensor.shape[-1] // 2
    freq = THETA ** (-(jnp.arange(half, dtype=jnp.float32) * 2.0 / tensor.shape[-1]))
    angle = offsets.astype(jnp.float32)[:, None] * freq[None, :]
    cosine = jnp.cos(angle)[:, None, :]
    sine = jnp.sin(angle)[:, None, :]
    first = tensor[..., :half]
    second = tensor[..., half:]
    return jnp.concatenate(
        [first * cosine - second * sine, second * cosine + first * sine], axis=-1
    )


def combine_stats(left, right):
    top = jnp.maximum(left[0], right[0])
    total = left[1] * jnp.exp(left[0] - top) + right[1] * jnp.exp(right[0] - top)
    return (top, total, left[2] + right[2])


def block_stats(scores, allowed):
    row_peak = jnp.max(scores, axis=-1)
    lifted = jnp.where(allowed[None, None, :, :], jnp.exp(scores - row_peak[..., None]), 0.0)
    return (row_peak, jnp.sum(lifted, axis=-1))


def weighted_values(scores, row_peak, row_total, value_block):
    safe_total = jnp.where(row_total > 0.0, row_total, 1.0)
    weights = (jnp.exp(scores - row_peak[..., None]) / safe_total[..., None]).astype(jnp.bfloat16)
    return jnp.einsum("ngck,knd->cngd", weights, value_block, preferred_element_type=jnp.float32)


def gathered_weights(
    hidden,
    segment_ids,
    targets,
    loss_mask,
    attn_gain,
    final_gain,
    w_query,
    w_key,
    w_value,
    w_out,
    head,
):
    tokens = hidden.shape[1]
    seq_index = lax.axis_index("seq")
    base = seq_index * tokens
    position = base + jnp.arange(tokens, dtype=jnp.int32)
    whole = lax.all_gather(hidden[0], "tp", axis=1, tiled=True)
    xfloat = whole.astype(jnp.float32)
    normed = rms_norm(xfloat, attn_gain[0]).astype(jnp.bfloat16)
    labels = jnp.arange(SEGMENTS, dtype=jnp.int32)
    member = segment_ids[None, :] == labels[:, None]
    local_first = jnp.min(jnp.where(member, position[None, :], FARTHEST), axis=1)
    starts = lax.pmin(local_first, "seq")
    token_start = jnp.sum(jnp.where(member, starts[:, None], 0), axis=0)
    offsets = position - token_start
    ranking = jnp.cumsum(loss_mask) - 1
    picks = (loss_mask[None, :] == 1) & (
        ranking[None, :] == jnp.arange(CAP, dtype=jnp.int32)[:, None]
    )
    chooser = picks.astype(jnp.bfloat16)
    normed_rows = jnp.dot(chooser, normed, preferred_element_type=jnp.float32).astype(jnp.bfloat16)
    x_rows = jnp.dot(chooser, whole, preferred_element_type=jnp.float32)
    row_pos = jnp.sum(jnp.where(picks, position[None, :], 0), axis=1)
    row_start = jnp.sum(jnp.where(picks, token_start[None, :], 0), axis=1)
    row_target = jnp.sum(jnp.where(picks, targets[None, :], 0), axis=1)
    places = jnp.stack([row_pos, row_start])
    query_cols = w_query.shape[2]
    key_cols = w_key.shape[2]
    local_heads = query_cols // HEAD_DIM
    local_kv = key_cols // HEAD_DIM
    group = local_heads // local_kv
    score_scale = HEAD_DIM ** (-0.5)
    query = jnp.dot(
        normed_rows,
        lax.all_gather(w_query[0], "seq", axis=0, tiled=True),
        preferred_element_type=jnp.float32,
    )
    keys = jnp.dot(
        normed,
        lax.all_gather(w_key[0], "seq", axis=0, tiled=True),
        preferred_element_type=jnp.float32,
    )
    values = jnp.dot(
        normed,
        lax.all_gather(w_value[0], "seq", axis=0, tiled=True),
        preferred_element_type=jnp.float32,
    )
    query = rotate(query.reshape(CAP, local_heads, HEAD_DIM), row_pos - row_start).astype(
        jnp.bfloat16
    )
    keys = rotate(keys.reshape(tokens, local_kv, HEAD_DIM), offsets).astype(jnp.bfloat16)
    values = values.reshape(tokens, local_kv, HEAD_DIM).astype(jnp.bfloat16)

    def masked_scores(query_rows, bounds, key_block, key_base):
        key_pos = key_base + jnp.arange(key_block.shape[0], dtype=jnp.int32)
        row_at = bounds[0][:, None]
        allowed = (key_pos[None, :] <= row_at) & (row_at - key_pos[None, :] < WINDOW)
        allowed = allowed & (key_pos[None, :] >= bounds[1][:, None])
        grouped = query_rows.reshape(CAP, local_kv, group, HEAD_DIM)
        scores = (
            jnp.einsum("cngd,knd->ngck", grouped, key_block, preferred_element_type=jnp.float32)
            * score_scale
        )
        return (jnp.where(allowed[None, None, :, :], scores, -1e30), allowed)

    reach = min(WINDOW // tokens, lax.axis_size("seq") - 1)
    own_scores, own_allowed = masked_scores(query, places, keys, base)
    row_peak, row_total = block_stats(own_scores, own_allowed)
    visited = []
    for step in range(1, reach + 1):
        guest = passed_along(query, "seq", -step)
        guest_places = passed_along(places, "seq", -step)
        guest_scores, guest_allowed = masked_scores(guest, guest_places, keys, base)
        guest_peak, guest_total = block_stats(guest_scores, guest_allowed)
        returned = passed_along(jnp.stack([guest_peak, guest_total]), "seq", step)
        back_peak = jnp.where(seq_index >= step, returned[0], -1e30)
        merged_peak = jnp.maximum(row_peak, back_peak)
        row_total = row_total * jnp.exp(row_peak - merged_peak) + returned[1] * jnp.exp(
            back_peak - merged_peak
        )
        row_peak = merged_peak
        visited.append(guest_scores)
    attended = weighted_values(own_scores, row_peak, row_total, values)
    for step in range(1, reach + 1):
        guest_stats = passed_along(jnp.stack([row_peak, row_total]), "seq", -step)
        share = weighted_values(visited[step - 1], guest_stats[0], guest_stats[1], values)
        attended = attended + passed_along(share, "seq", step)
    attended = attended.astype(jnp.bfloat16).reshape(CAP, query_cols)
    partial_out = jnp.dot(
        attended,
        lax.all_gather(w_out[0], "seq", axis=1, tiled=True),
        preferred_element_type=jnp.float32,
    )
    summed = lax.psum(partial_out, "tp")
    state = x_rows + summed
    final = rms_norm(state, final_gain[0]).astype(jnp.bfloat16)
    all_rows = lax.all_gather(final, "seq", axis=0, tiled=True)
    all_targets = lax.all_gather(row_target, "seq", axis=0, tiled=True)
    logits = jnp.dot(all_rows, head[0], preferred_element_type=jnp.float32)
    vocab_start = (seq_index * lax.axis_size("tp") + lax.axis_index("tp")) * head.shape[2]
    local_top = jnp.max(logits, axis=1)
    local_total = jnp.sum(jnp.exp(logits - local_top[:, None]), axis=1)
    hit = all_targets[:, None] == vocab_start + jnp.arange(head.shape[2], dtype=jnp.int32)[None, :]
    local_target = jnp.sum(jnp.where(hit, logits, 0.0), axis=1)
    merged_top, merged_total, merged_target = joined(
        (local_top, local_total, local_target), ("seq", "tp"), combine_stats
    )
    logp = merged_target - (merged_top + jnp.log(merged_total))
    own = lax.dynamic_slice_in_dim(logp, seq_index * CAP, CAP, 0)
    placed = jnp.sum(jnp.where(picks, own[:, None], 0.0), axis=0)
    return placed[None, :].astype(jnp.float32)


def place():
    return lax.axis_index("seq"), lax.axis_index("tp")


def greet(peers):
    barrier = pltpu.get_barrier_semaphore()
    for peer in peers:
        pl.semaphore_signal(barrier, inc=1, device_id=peer, device_id_type=pl.DeviceIdType.MESH)
    pl.semaphore_wait(barrier, len(peers))


def remote(source, target, send, recv, peer):
    return pltpu.make_async_remote_copy(
        src_ref=source,
        dst_ref=target,
        send_sem=send,
        recv_sem=recv,
        device_id=peer,
        device_id_type=pl.DeviceIdType.MESH,
    )


def everyone(seq, tp):
    s, t = place()
    return [
        ((d, e), {"seq": lax.rem(s + d, seq), "tp": lax.rem(t + e, tp)})
        for d in range(seq)
        for e in range(tp)
        if (d, e) != (0, 0)
    ]


def tell_all(seq, tp, value, out, send, recv):
    s, t = place()
    out[s, t] = value[...]
    copies = []
    for number, (_, peer) in enumerate(everyone(seq, tp)):
        copy = remote(value, out.at[s, t], send.at[number], recv.at[number], peer)
        copy.start()
        copies.append(copy)
    return copies


def fused_kernel(
    seq,
    x,
    segs,
    mask,
    target_ids,
    freq,
    attn_gain,
    final_gain,
    wq_hbm,
    wk_hbm,
    wv_hbm,
    wo_hbm,
    head_hbm,
    out,
    wq,
    wk,
    wv,
    wo,
    head,
    meta,
    told,
    sums,
    sumtold,
    half,
    blocks,
    parts,
    inbox,
    qparts,
    qinbox,
    picks,
    rowinfo,
    scales,
    tables,
    keys,
    values,
    queries,
    att,
    rawrows,
    away,
    arrived_away,
    here,
    fin,
    logits,
    squares,
    sqtold,
    stats,
    sttold,
    wsem,
    xsend,
    xrecv,
    send,
    recv,
    fsend,
    frecv,
    msend,
    mrecv,
    usend,
    urecv,
    csend,
    crecv,
    qsend,
    qrecv,
    asend,
    arecv,
    esend,
    erecv,
    zsend,
    zrecv,
    bsend,
    brecv,
    sqsend,
    sqrecv,
    stsend,
    strecv,
):
    f32, bf16 = jnp.float32, jnp.bfloat16
    s, t = place()
    other = 1 - t
    side = s // 2
    is_end = jnp.logical_or(s == 0, s == seq - 1)
    is_mid = jnp.logical_not(is_end)
    home = side == t
    tokens = x.shape[0]
    model = x.shape[1] * 2
    rows = tokens // 4
    width = model // seq
    beside = {"seq": s, "tp": other}
    dot = functools.partial(jnp.dot, preferred_element_type=f32)

    loads = [
        pltpu.make_async_copy(a, b, wsem.at[i])
        for i, (a, b) in enumerate(
            ((wk_hbm, wk), (wv_hbm, wv), (wq_hbm, wq), (wo_hbm, wo), (head_hbm, head))
        )
    ]
    for load in loads:
        load.start()
    greet([peer for _, peer in everyone(seq, 2)])
    meta[0:1, :] = segs[...].astype(f32)
    meta[1:2, :] = mask[...].astype(f32)
    meta[2:3, :] = target_ids[...].astype(f32)
    meta[3:8, :] = jnp.zeros((5, tokens), f32)
    messages = tell_all(seq, 2, meta, told, msend, mrecv)

    def piece(which, p, i):
        at = pl.multiple_of((which * 2 + p) * rows, rows)
        return x.at[pl.ds(at, rows), pl.ds(i * width, width)]

    def got(p, i):
        return half.at[p, :, pl.ds(i * width, width)]

    pairs = [(p, i) for p in range(2) for i in range(2)]
    firsts = {
        (p, i): remote(piece(other, p, i), got(p, i), xsend.at[p, i], xrecv.at[p, i], beside)
        for p, i in pairs
    }
    for pair in pairs:
        firsts[pair].start()

    def arrived(source, p):
        block = blocks.at[source, t * 2 + p]
        return remote(block, block, send.at[source, p], recv.at[source, p], beside)

    def passed(source, p):
        block = blocks.at[source, t * 2 + p]
        return remote(block, block, fsend.at[source, p], frecv.at[source, p], beside)

    def hand(view, target, p):
        remote(
            view, blocks.at[s, t * 2 + p], send.at[target, p], recv.at[s, p], {"seq": target, "tp": t}
        ).start()

    for p, i in pairs:
        target = t * 2 + i

        @pl.when(target != s)
        def _():
            hand(piece(t, p, i), target, p)

        @pl.when(target == s)
        def _():
            remote(
                piece(t, p, i), blocks.at[s, t * 2 + p], fsend.at[s, p], frecv.at[s, p], beside
            ).start()
            blocks[s, t * 2 + p] = piece(t, p, i)[...]
            blocks[s, other * 2 + p] = piece(other, p, i)[...]

    fold = jnp.zeros((tokens, 128), f32)
    for c in range(x.shape[1] // 128):
        part = x[:, c * 128 : (c + 1) * 128].astype(f32)
        fold = fold + part * part
    sums[...] = jnp.broadcast_to(jnp.sum(fold.T, axis=0, keepdims=True), sums.shape)
    summessages = tell_all(seq, 2, sums, sumtold, usend, urecv)
    for p, i in pairs:
        firsts[p, i].wait_recv()
        target = other * 2 + i

        @pl.when(target != s)
        def _():
            hand(got(p, i), target, p)

        @pl.when(target == s)
        def _():
            blocks[s, t * 2 + p] = got(p, i)[...]

    for message in messages:
        message.wait_recv()

    upper = lax.broadcasted_iota(jnp.int32, (tokens, tokens), 0)
    upper = (upper <= lax.broadcasted_iota(jnp.int32, (tokens, tokens), 1)).astype(f32).astype(bf16)
    spot = lax.broadcasted_iota(jnp.int32, (1, tokens), 1).astype(f32)
    order = lax.broadcasted_iota(jnp.int32, (CAP, tokens), 0).astype(f32) + 1.0
    begins = [jnp.full((1, 1), float(FARTHEST), f32) for _ in range(SEGMENTS)]
    for b in range(seq):
        seg = told[b, 0, 0:1, :]
        for j in range(SEGMENTS):
            low = jnp.where(seg == float(j), spot + float(b * tokens), float(FARTHEST))
            begins[j] = jnp.minimum(begins[j], jnp.min(low, axis=1, keepdims=True))
    for b in range(seq):
        chosen = told[b, 0, 1:2, :]
        rank = dot(jnp.broadcast_to(chosen, (8, tokens)).astype(bf16), upper)[0:1, :]
        hit = jnp.logical_and(chosen == 1.0, rank == order)
        picks[b] = jnp.where(hit, 1.0, 0.0).astype(bf16)

        def column(line):
            return jnp.sum(jnp.where(hit, line, 0.0), axis=1, keepdims=True)

        seg = column(told[b, 0, 0:1, :])
        begin = jnp.zeros((CAP, 1), f32)
        for j in range(SEGMENTS):
            begin = begin + jnp.where(seg == float(j), begins[j], 0.0)
        here_rows = slice(b * CAP, (b + 1) * CAP)
        info = (column(spot + float(b * tokens)), begin, column(told[b, 0, 2:3, :]))
        for kind, value in enumerate(info):
            rowinfo[kind, here_rows] = jnp.broadcast_to(value, (CAP, 128))

    gain = attn_gain[0:1, pl.ds(pl.multiple_of(s * width, width), width)]
    for load in loads[:3]:
        load.wait()
    kcols = wk.shape[1] // 2
    qcols = wq.shape[1] // 2
    partner = s + 1 - 2 * lax.rem(s, 2)
    near, far = 2 - side, 3 * (1 - side)

    def choose(number, options):
        value = options[-1]
        for k in range(len(options) - 2, -1, -1):
            value = jnp.where(number == k, options[k], value)
        return value

    def pick_from(number, codes):
        code = choose(number, codes)
        return choose(code // 4, (s, partner, near, far)), jnp.where(
            lax.rem(code, 4) < 2, t * 2 + lax.rem(code, 4), other * 2 + lax.rem(code, 4) - 2
        ), lax.rem(code, 4)

    def tok_ship(d, source, g):
        peer = {"seq": lax.rem(s + 2 * d - 1 + seq, seq), "tp": t}
        chunk = source * 4 + g
        return remote(
            parts.at[d, chunk], inbox.at[d, chunk], csend.at[d, chunk], crecv.at[d, chunk], peer
        )

    def que_ship(d, source):
        peer = {"seq": lax.rem(s + 2 * d - 1 + seq, seq), "tp": t}
        return remote(
            qparts.at[d, source], qinbox.at[d, source], qsend.at[d, source], qrecv.at[d, source], peer
        )

    def ship(d, source, g, last):
        tok_ship(d, source, g).start()

        @pl.when(last)
        def _():
            que_ship(d, source).start()

    def await_ship(d, source, g, last):
        tok_ship(d, source, g).wait_recv()

        @pl.when(last)
        def _():
            que_ship(d, source).wait_recv()

    def project(source, g, last):
        block = (blocks[source, g].astype(f32) * gain).astype(bf16)
        chunk = source * 4 + g
        for d in range(2):
            cols = slice(d * kcols, (d + 1) * kcols)
            parts[d, chunk, :, :kcols] = dot(block, wk[:, cols]).astype(bf16)
            parts[d, chunk, :, kcols:] = dot(block, wv[:, cols]).astype(bf16)

        @pl.when(last)
        def _():
            raw = dot(picks[source], blocks[source].reshape(tokens, width))
            rawrows[source] = raw.astype(bf16)
            taken = (raw * gain).astype(bf16)
            for d in range(2):
                cols = slice(d * qcols, (d + 1) * qcols)
                qparts[d, source] = dot(taken, wq[:, cols]).astype(bf16)

        @pl.when(is_end)
        def _():
            ship(1 - side, source, g, last)

    def combine(d, source, g, last):
        await_ship(d, source, g, last)
        chunk = source * 4 + g
        both = parts[d, chunk].astype(f32) + inbox[d, chunk].astype(f32)
        parts[d, chunk] = both.astype(bf16)

        @pl.when(last)
        def _():
            both = qparts[d, source].astype(f32) + qinbox[d, source].astype(f32)
            qparts[d, source] = both.astype(bf16)

        ship(d, source, g, last)

    chunks = 4 * seq
    order_own = (0, 12, 1, 2, 4, 13, 3, 5, 14, 8, 6, 15, 9, 7, 10, 11)
    order_one = (12, 0, 4, 13, 1, 5, 14, 8, 2, 6, 15, 9, 3, 7, 10, 11)
    order_two = (4, 12, 5, 8, 13, 9, 6, 0, 10, 14, 7, 1, 11, 15, 2, 3)
    order_end = (0, 12, 1, 8, 13, 9, 2, 4, 10, 14, 3, 5, 11, 15, 6, 7)
    lag_one, lag_two = 4, 7

    def step(number, carry):
        @pl.when(number < chunks)
        def _():
            source, g, kind = pick_from(number, order_own)

            @pl.when(jnp.logical_and(kind < 2, source != s))
            def _():
                arrived(source, kind).wait_recv()
                passed(source, kind).start()

            awaits = jnp.logical_not(jnp.logical_and(source == s, home))

            @pl.when(jnp.logical_and(kind >= 2, awaits))
            def _():
                passed(source, kind - 2).wait_recv()

            project(source, g, kind == 3)

        one = number - lag_one

        @pl.when(jnp.logical_and(is_mid, jnp.logical_and(one >= 0, one < chunks)))
        def _():
            source, g, kind = pick_from(one, order_one)
            combine(1 - side, source, g, kind == 3)

        two = number - lag_two

        @pl.when(jnp.logical_and(is_mid, jnp.logical_and(two >= 0, two < chunks)))
        def _():
            source, g, kind = pick_from(two, order_two)
            combine(side, source, g, kind == 3)

        return carry

    lax.fori_loop(0, chunks + lag_two, step, 0)

    for message in summessages:
        message.wait_recv()
    for b in range(seq):
        scale = lax.rsqrt((sumtold[b, 0, 0:1, :] + sumtold[b, 1, 0:1, :]) / model + EPS)
        scales[0:1, b * tokens : (b + 1) * tokens] = scale
        value = jnp.sum(picks[b].astype(f32) * scale, axis=1, keepdims=True)
        rowinfo[3, b * CAP : (b + 1) * CAP] = jnp.broadcast_to(value, (CAP, 128))
    def turned(values, cosine, sine):
        return values * cosine + pltpu.roll(values, HEAD_DIM // 2, 1) * sine

    per = seq // 2

    def tell(b, hop):
        peer = {"seq": s + hop * (1 - 2 * side), "tp": t}
        block = att.at[side, b]
        return remote(block, block, asend.at[b, hop], arecv.at[side, b], peer)

    def told_of(source_side, b):
        block = att.at[source_side, b]
        return remote(block, block, asend.at[b, 0], arecv.at[source_side, b], beside)

    def cross(i):
        return remote(away.at[i], arrived_away.at[i], esend.at[i], erecv.at[i], beside)

    length = seq * tokens
    sign = jnp.where(lax.broadcasted_iota(jnp.int32, (1, HEAD_DIM), 1) < HEAD_DIM // 2, -1.0, 1.0)
    kv = kcols // HEAD_DIM
    group = qcols // kcols

    @pl.when(is_end)
    def _():
        def table(b, carry):
            at = pl.ds(pl.multiple_of(b * rows, rows), rows)
            line = lax.broadcasted_iota(jnp.int32, (rows, HEAD_DIM), 0) + b * rows
            angle = line.astype(f32) * freq[...]
            tables[0, at] = jnp.cos(angle)
            tables[1, at] = jnp.sin(angle) * sign
            return carry

        lax.fori_loop(0, length // rows, table, 0)
        angle = rowinfo[0] * freq[...]
        tables[0, length:] = jnp.cos(angle)
        tables[1, length:] = jnp.sin(angle) * sign

        def settle(number, carry):
            source, g, kind = pick_from(number, order_end)
            await_ship(side, source, g, kind == 3)
            chunk = source * 4 + g
            both = parts[side, chunk].astype(f32) + inbox[side, chunk].astype(f32)
            at = pl.ds(pl.multiple_of(chunk * rows, rows), rows)
            cosine, sine = tables[0, at], tables[1, at]
            for j in range(kv):
                key = both[:, j * HEAD_DIM : (j + 1) * HEAD_DIM]
                keys[j, at] = turned(key, cosine, sine).astype(bf16)
                values[j, at] = both[:, kcols + j * HEAD_DIM : kcols + (j + 1) * HEAD_DIM].astype(bf16)

            @pl.when(kind == 3)
            def _():
                both = qparts[side, source].astype(f32) + qinbox[side, source].astype(f32)
                at = pl.ds(pl.multiple_of(source * CAP, CAP), CAP)
                far_at = pl.ds(pl.multiple_of(length + source * CAP, CAP), CAP)
                cosine, sine = tables[0, far_at], tables[1, far_at]
                both = both * rowinfo[3, at][:, 0:1]
                for j in range(kv * group):
                    query = both[:, j * HEAD_DIM : (j + 1) * HEAD_DIM]
                    queries[j, at] = turned(query, cosine, sine).astype(bf16)

            return carry

        lax.fori_loop(0, chunks, settle, 0)
        position = lax.broadcasted_iota(jnp.int32, (1, length), 1).astype(f32)
        scale = scales[0:1, :]
        for which in (other, t):
            at = pl.ds(pl.multiple_of(which * per * CAP, per * CAP), per * CAP)
            row_at, row_start = rowinfo[0, at][:, 0:1], rowinfo[1, at][:, 0:1]
            allowed = jnp.logical_and(position <= row_at, position >= row_start)
            allowed = jnp.logical_and(allowed, row_at - position < float(WINDOW))
            for j in range(kv * group):
                scores = lax.dot_general(
                    queries[j, at], keys[j // group], (((1,), (1,)), ((), ())), preferred_element_type=f32
                )
                scores = jnp.where(allowed, scores * (scale * HEAD_DIM ** (-0.5)), -1e30)
                lifted = jnp.exp(scores - jnp.max(scores, axis=1, keepdims=True))
                lifted = lifted * (1.0 / jnp.sum(lifted, axis=1, keepdims=True))
                result = dot((lifted * scale).astype(bf16), values[j // group]).astype(bf16)
                for b in range(per):
                    cols = slice(j * HEAD_DIM, (j + 1) * HEAD_DIM)
                    att[side, which * per + b, :, cols] = result[b * CAP : (b + 1) * CAP]
            for b in range(per):
                for hop in range(seq - 1, 0, -1):
                    tell(which * per + b, hop).start()

    loads[3].wait()
    late_gain = final_gain[0:1, pl.ds(pl.multiple_of(s * width, width), width)]
    turns = [other * per, other * per + 1, t * per, t * per + 1]
    for k, b in enumerate(turns):
        for source_side in range(2):

            @pl.when(s != (seq - 1) * source_side)
            def _():
                told_of(source_side, b).wait_recv()

        result = dot(att[0, b], wo[:qcols]) + dot(att[1, b], wo[qcols:])
        if k < per:
            away[k] = result.astype(bf16)
            cross(k).start()
        else:
            here[k - per] = result + rawrows[b].astype(f32)

    def along(source, target, i):
        block = fin.at[source, t, i]
        return remote(
            block, block, zsend.at[i, target], zrecv.at[source, i], {"seq": target, "tp": t}
        )

    def onward(i):
        block = fin.at[far, t, i]
        return remote(
            block, block, zsend.at[i, seq], zrecv.at[far, i], {"seq": partner, "tp": t}
        )

    def across(source, i):
        return remote(
            fin.at[source, t, i], fin.at[source, t, i], bsend.at[source, i], brecv.at[source, i], beside
        )

    fold = []
    for i in range(per):
        cross(i).wait_recv()
        state = here[i] + arrived_away[i].astype(f32)
        fin[s, t, i] = (state * late_gain).astype(bf16)
        across(s, i).start()
        for hop in range(1, seq - 1):
            for d in range(2):
                target = s + hop * (2 * d - 1)

                @pl.when(jnp.logical_and(target >= 0, target < seq))
                def _():
                    along(s, target, i).start()

        total = jnp.zeros((CAP, 128), f32)
        for c in range(width // 128):
            part = state[:, c * 128 : (c + 1) * 128]
            total = total + part * part
        fold.append(total)
    zero = jnp.zeros((CAP, 128), f32)
    lower = t == 0
    fold = [jnp.where(lower, v, zero) for v in fold] + [jnp.where(lower, zero, v) for v in fold]
    total = jnp.concatenate(fold, axis=0)
    squares[...] = jnp.broadcast_to(jnp.sum(total.T, axis=0, keepdims=True), squares.shape)
    sqmessages = tell_all(seq, 2, squares, sqtold, sqsend, sqrecv)
    loads[4].wait()

    def add(source, which, fresh):
        at = pl.ds(pl.multiple_of(which * per * CAP, per * CAP), per * CAP)
        weight = head[pl.ds(pl.multiple_of(source * width, width), width)]
        value = dot(fin[source, which].reshape(per * CAP, width), weight)
        logits[at] = value if fresh else logits[at] + value

    sources = [s - hop * (2 * d - 1) for hop in range(1, seq) for d in range(2)]
    valid = [jnp.logical_and(source >= 0, source < seq) for source in sources]
    add(s, t, True)
    for i in range(per):
        for source, good in zip(sources, valid):

            @pl.when(good)
            def _():
                along(source, s, i).wait_recv()

                @pl.when(jnp.logical_and(is_mid, source == far))
                def _():
                    onward(i).start()

                across(source, i).start()

    for source, good in zip(sources, valid):

        @pl.when(good)
        def _():
            add(source, t, False)

    for i in range(per):
        across(s, i).wait_recv()
    add(s, other, True)
    for source, good in zip(sources, valid):

        @pl.when(good)
        def _():
            for i in range(per):
                across(source, i).wait_recv()
            add(source, other, False)

    for message in sqmessages:
        message.wait_recv()
    total = jnp.zeros(squares.shape, f32)
    for b in range(seq):
        total = total + sqtold[b, 0] + sqtold[b, 1]
    count = seq * CAP
    mean = jnp.broadcast_to(total[0:1, :], (count, count)).T[:, 0:1] / model
    final = logits[...] * lax.rsqrt(mean + EPS)
    entries = final.shape[1]
    top = jnp.max(final, axis=1, keepdims=True)
    exps = jnp.sum(jnp.exp(final - top), axis=1, keepdims=True)
    label = lax.broadcasted_iota(jnp.int32, (1, entries), 1) + (s * 2 + t) * entries
    found = jnp.sum(
        jnp.where(rowinfo[2][:, 0:1] == label.astype(f32), final, 0.0), axis=1, keepdims=True
    )
    lane = lax.broadcasted_iota(jnp.int32, (count, count), 1)
    packed = jnp.where(lane == 0, top, jnp.where(lane == 1, exps, jnp.where(lane == 2, found, 0.0)))
    stats[...] = packed.T[0:8, :]
    stmessages = tell_all(seq, 2, stats, sttold, stsend, strecv)
    for message in stmessages:
        message.wait_recv()
    everyones = [sttold[b, e] for b in range(seq) for e in range(2)]
    best = everyones[0][0:1, :]
    for value in everyones[1:]:
        best = jnp.maximum(best, value[0:1, :])
    summed = jnp.zeros((1, count), f32)
    hits = jnp.zeros((1, count), f32)
    for value in everyones:
        summed = summed + value[1:2, :] * jnp.exp(value[0:1, :] - best)
        hits = hits + value[2:3, :]
    logp = hits - (best + jnp.log(summed))
    own = picks[s].astype(f32)
    select = jnp.concatenate([jnp.where(s == b, own, 0.0) for b in range(seq)], axis=0)
    column = jnp.broadcast_to(logp, (count, count)).T[:, 0:1]
    out[...] = jnp.sum(select * column, axis=0, keepdims=True)

    for pair in pairs:
        firsts[pair].wait_send()
    for source in range(seq):
        for p in range(2):

            @pl.when(source != s)
            def _():
                arrived(source, p).wait_send()

            @pl.when(jnp.logical_or(source != s, home))
            def _():
                passed(source, p).wait_send()

    for message in messages + summessages + sqmessages + stmessages:
        message.wait_send()
    for d in range(2):

        @pl.when(s != (seq - 1) * d)
        def _():
            for source in range(seq):
                for g in range(4):
                    tok_ship(d, source, g).wait_send()
                que_ship(d, source).wait_send()

    @pl.when(is_end)
    def _():
        for b in range(seq):
            for hop in range(1, seq):
                tell(b, hop).wait_send()

    for i in range(per):
        cross(i).wait_send()
        for source in range(seq):
            across(source, i).wait_send()

            @pl.when(jnp.logical_and(source != s, jnp.abs(source - s) < seq - 1))
            def _():
                along(s, source, i).wait_send()

        @pl.when(is_mid)
        def _():
            onward(i).wait_send()


def fused_rows(
    hidden,
    segment_ids,
    targets,
    loss_mask,
    attn_gain,
    final_gain,
    w_query,
    w_key,
    w_value,
    w_out,
    head,
):
    seq = lax.axis_size("seq")
    tokens, features = hidden.shape[1:]
    model = features * 2
    width = w_key.shape[1]
    rows = tokens // 4
    kcols = w_key.shape[2] // 2
    qcols = w_query.shape[2] // 2
    kv = kcols // HEAD_DIM
    entries = head.shape[2]
    count = seq * CAP
    freq = THETA ** (-(np.arange(HEAD_DIM // 2) * 2.0 / HEAD_DIM))
    freq = jnp.asarray(np.concatenate([freq, freq])[None, :].astype(np.float32))
    vmem = pl.BlockSpec(memory_space=pltpu.VMEM)
    hbm = pl.BlockSpec(memory_space=pl.ANY)
    bf16, f32 = jnp.bfloat16, jnp.float32
    dma = pltpu.SemaphoreType.DMA
    return pl.pallas_call(
        functools.partial(fused_kernel, seq),
        out_shape=jax.ShapeDtypeStruct((1, tokens), f32),
        in_specs=[vmem] * 7 + [hbm] * 5,
        out_specs=vmem,
        scratch_shapes=[
            pltpu.VMEM(w_query.shape[1:], bf16),
            pltpu.VMEM(w_key.shape[1:], bf16),
            pltpu.VMEM(w_value.shape[1:], bf16),
            pltpu.VMEM(w_out.shape[1:], bf16),
            pltpu.VMEM(head.shape[1:], bf16),
            pltpu.VMEM((8, tokens), f32),
            pltpu.VMEM((seq, 2, 8, tokens), f32),
            pltpu.VMEM((8, tokens), f32),
            pltpu.VMEM((seq, 2, 8, tokens), f32),
            pltpu.VMEM((2, rows, features), bf16),
            pltpu.VMEM((seq, 4, rows, width), bf16),
            pltpu.VMEM((2, 4 * seq, rows, 2 * kcols), bf16),
            pltpu.VMEM((2, 4 * seq, rows, 2 * kcols), bf16),
            pltpu.VMEM((2, seq, CAP, qcols), bf16),
            pltpu.VMEM((2, seq, CAP, qcols), bf16),
            pltpu.VMEM((seq, CAP, tokens), bf16),
            pltpu.VMEM((4, count, 128), f32),
            pltpu.VMEM((8, seq * tokens), f32),
            pltpu.VMEM((2, seq * tokens + count, HEAD_DIM), f32),
            pltpu.VMEM((kv, seq * tokens, HEAD_DIM), bf16),
            pltpu.VMEM((kv, seq * tokens, HEAD_DIM), bf16),
            pltpu.VMEM((qcols // HEAD_DIM, count, HEAD_DIM), bf16),
            pltpu.VMEM((2, seq, CAP, qcols), bf16),
            pltpu.VMEM((seq, CAP, width), bf16),
            pltpu.VMEM((seq // 2, CAP, width), bf16),
            pltpu.VMEM((seq // 2, CAP, width), bf16),
            pltpu.VMEM((seq // 2, CAP, width), f32),
            pltpu.VMEM((seq, 2, seq // 2, CAP, width), bf16),
            pltpu.VMEM((count, entries), f32),
            pltpu.VMEM((8, count), f32),
            pltpu.VMEM((seq, 2, 8, count), f32),
            pltpu.VMEM((8, count), f32),
            pltpu.VMEM((seq, 2, 8, count), f32),
            dma((5,)),
            dma((2, 2)),
            dma((2, 2)),
            dma((seq, 2)),
            dma((seq, 2)),
            dma((seq, 2)),
            dma((seq, 2)),
            dma((2 * seq,)),
            dma((2 * seq,)),
            dma((2 * seq,)),
            dma((2 * seq,)),
            dma((2, 4 * seq)),
            dma((2, 4 * seq)),
            dma((2, seq)),
            dma((2, seq)),
            dma((seq, seq)),
            dma((2, seq)),
            dma((seq // 2,)),
            dma((seq // 2,)),
            dma((seq // 2, seq + 1)),
            dma((seq, seq // 2)),
            dma((seq, seq // 2)),
            dma((seq, seq // 2)),
            dma((2 * seq,)),
            dma((2 * seq,)),
            dma((2 * seq,)),
            dma((2 * seq,)),
        ],
        compiler_params=pltpu.CompilerParams(collective_id=0, has_side_effects=True),
    )(
        hidden[0],
        segment_ids[None, :],
        loss_mask[None, :],
        targets[None, :],
        freq,
        attn_gain,
        final_gain,
        w_query[0],
        w_key[0],
        w_value[0],
        w_out[0],
        head[0],
    )


def solution(mesh):
    placed = (
        P("ref", ("groups", "seq"), "tp"),
        P(("groups", "seq")),
        P(("groups", "seq")),
        P(("groups", "seq")),
        P("ref", None),
        P("ref", None),
        P("ref", "seq", "tp"),
        P("ref", "seq", "tp"),
        P("ref", "seq", "tp"),
        P("ref", "tp", "seq"),
        P("ref", None, ("seq", "tp")),
    )

    def shards(*args):
        seq, tp = mesh.shape["seq"], mesh.shape["tp"]
        own_heads = args[7].shape[2] // HEAD_DIM
        moves = tp == 2 and seq == 4 and own_heads == seq and args[6].shape[2] == 2 * args[7].shape[2]
        return (fused_rows if moves else gathered_weights)(*args)

    return jax.shard_map(
        shards, mesh=mesh, in_specs=placed, out_specs=P("ref", ("groups", "seq")), check_vma=False
    )
```
